32 devices in a mesh: dp: 1 (over z), cp: 32 (over y, x, core).
Axes of the slice: x: 4, y: 4, z: 1, core: 2. Of those that a mesh axis runs over, the one named last changes fastest.
The devices are a block of a 4x4x8 slice.
Arguments:
- hidden: bfloat16 [6, 4096, 4096], P('dp', 'cp')
- positions: int32 [6, 4096], P('dp', 'cp')
- norm_gain: bfloat16 [4096], replicated
- w_query: bfloat16 [4096, 4096], replicated
- w_key: bfloat16 [4096, 1024], replicated
- w_value: bfloat16 [4096, 1024], replicated
- w_out: bfloat16 [32, 128, 4096], replicated
Outputs:
- output: bfloat16 [6, 4096, 4096], P('dp', 'cp')
All inputs are finite; a program needn't handle non-finite values.
Results may differ from the reference program's by a relative error of at most 0.00731925.
Values are sent between devices in bfloat16 or wider.
A program may use at most 768 MiB of HBM per device.

```python
import jax
import jax.numpy as jnp
from jax import lax

BATCH = 6
SEQ = 4096
QBLOCK = 128
D = 4096
HEADS = 32
KV_HEADS = 8
HEAD = 128

GROUPS = HEADS // KV_HEADS
NBLOCKS = SEQ // QBLOCK


def draw_positions(pos_key):
    off_key, stride_key = jax.random.split(pos_key)
    offsets = jax.random.randint(off_key, (BATCH, 1), 0, SEQ)
    strides = jax.random.randint(stride_key, (BATCH, SEQ), 1, 3)
    return (offsets + jnp.cumsum(strides, axis=1) - 1).astype(jnp.int32)


def normal_weight(weight_key, shape, scale):
    return (scale * jax.random.normal(weight_key, shape, jnp.float32)).astype(jnp.bfloat16)


def setup_inputs(seed: int = 0, part: int = 0) -> dict:
    root = jax.random.key(seed)
    part_key = jax.random.fold_in(root, part)
    shared = jax.random.fold_in(root, 1000003)
    hid_key, pos_key = jax.random.split(part_key)
    gain_key, q_key, k_key, v_key, o_key = jax.random.split(shared, 5)
    hidden = (0.25 * jax.random.normal(hid_key, (BATCH, SEQ, D), jnp.float32)).astype(jnp.bfloat16)
    norm_gain = (1.0 + 0.3 * jax.random.normal(gain_key, (D,), jnp.float32)).astype(jnp.bfloat16)
    return {
        'hidden': hidden,
        'positions': draw_positions(pos_key),
        'norm_gain': norm_gain,
        'w_query': normal_weight(q_key, (D, HEADS * HEAD), 1.3 * D ** -0.5),
        'w_key': normal_weight(k_key, (D, KV_HEADS * HEAD), 1.3 * D ** -0.5),
        'w_value': normal_weight(v_key, (D, KV_HEADS * HEAD), D ** -0.5),
        'w_out': normal_weight(o_key, (HEADS, HEAD, D), 2.0 * (HEADS * HEAD) ** -0.5),
    }


def rms_norm(hidden, norm_gain):
    x_f32 = hidden.astype(jnp.float32)
    inv_rms = lax.rsqrt(jnp.mean(x_f32 * x_f32, axis=-1, keepdims=True) + 1e-5)
    return (x_f32 * inv_rms * norm_gain.astype(jnp.float32)).astype(jnp.bfloat16)


def rotary(proj_f32, positions):
    head_dim = proj_f32.shape[-1]
    half_dim = head_dim // 2
    inv_freq = 10000.0 ** (-2.0 * jnp.arange(half_dim, dtype=jnp.float32) / head_dim)
    angles = positions.astype(jnp.float32)[:, :, None] * inv_freq
    cos_part = jnp.cos(angles)[:, :, None, :]
    sin_part = jnp.sin(angles)[:, :, None, :]
    first_half = proj_f32[..., :half_dim]
    second_half = proj_f32[..., half_dim:]
    return jnp.concatenate([first_half * cos_part - second_half * sin_part, second_half * cos_part + first_half * sin_part], axis=-1).astype(jnp.bfloat16)


def reference(hidden, positions, norm_gain, w_query, w_key, w_value, w_out):
    normed = rms_norm(hidden, norm_gain).reshape(BATCH * SEQ, D)
    q_rot = rotary(jnp.dot(normed, w_query, preferred_element_type=jnp.float32).reshape(BATCH, SEQ, HEADS, HEAD), positions)
    k_rot = rotary(jnp.dot(normed, w_key, preferred_element_type=jnp.float32).reshape(BATCH, SEQ, KV_HEADS, HEAD), positions)
    v_all = jnp.dot(normed, w_value, preferred_element_type=jnp.float32).astype(jnp.bfloat16).reshape(BATCH, SEQ, KV_HEADS, HEAD)
    q_grp = q_rot.reshape(BATCH, SEQ, KV_HEADS, GROUPS, HEAD).astype(jnp.float32)
    k_f32 = k_rot.astype(jnp.float32)
    v_f32 = v_all.astype(jnp.float32)
    w_out_grp = w_out.reshape(KV_HEADS, GROUPS, HEAD, D).astype(jnp.float32)
    token_idx = jnp.arange(QBLOCK)

    def query_block(query_idx):
        q_blk = lax.dynamic_slice_in_dim(q_grp, query_idx * QBLOCK, QBLOCK, axis=1)

        def key_step(att_state, key_idx):
            def consume(state_in):
                run_max, run_sum, acc_out = state_in
                k_blk = lax.dynamic_slice_in_dim(k_f32, key_idx * QBLOCK, QBLOCK, axis=1)
                v_blk = lax.dynamic_slice_in_dim(v_f32, key_idx * QBLOCK, QBLOCK, axis=1)
                scores = jnp.einsum('bqkgd,bskd->bkgqs', q_blk, k_blk) * (HEAD ** -0.5)
                allowed = (query_idx * QBLOCK + token_idx)[:, None] >= (key_idx * QBLOCK + token_idx)[None, :]
                scores = jnp.where(allowed, scores, -jnp.inf)
                new_max = jnp.maximum(run_max, jnp.max(scores, axis=-1))
                prob_blk = jnp.exp(scores - new_max[..., None])
                rescale = jnp.exp(run_max - new_max)
                new_sum = run_sum * rescale + jnp.sum(prob_blk, axis=-1)
                new_acc = acc_out * rescale[..., None] + jnp.einsum('bkgqs,bskd->bkgqd', prob_blk, v_blk)
                return new_max, new_sum, new_acc
            return lax.cond(key_idx <= query_idx, consume, lambda state_kept: state_kept, att_state), None

        start_state = (
            jnp.full((BATCH, KV_HEADS, GROUPS, QBLOCK), -jnp.inf, jnp.float32),
            jnp.zeros((BATCH, KV_HEADS, GROUPS, QBLOCK), jnp.float32),
            jnp.zeros((BATCH, KV_HEADS, GROUPS, QBLOCK, HEAD), jnp.float32),
        )
        final_state, _ = lax.scan(key_step, start_state, jnp.arange(NBLOCKS))
        attn_out = (final_state[2] / final_state[1][..., None]).astype(jnp.bfloat16).astype(jnp.float32)
        x_blk = lax.dynamic_slice_in_dim(hidden, query_idx * QBLOCK, QBLOCK, axis=1).astype(jnp.float32)
        return (x_blk + jnp.einsum('bkgqd,kgde->bqe', attn_out, w_out_grp)).astype(jnp.bfloat16)

    out_blocks = lax.map(query_block, jnp.arange(NBLOCKS))
    return jnp.moveaxis(out_blocks, 0, 1).reshape(BATCH, SEQ, D)
```

```python
import functools

import jax
import jax.numpy as jnp
from jax import lax
from jax.experimental import pallas as pl
from jax.experimental.pallas import tpu as pltpu
from jax.sharding import PartitionSpec as P

AXIS = 'cp'
LOG2E = 1.4426950408889634
VMEM_LIMIT = 60 * 1024 * 1024


def rms_norm(hidden, norm_gain):
    x_f32 = hidden.astype(jnp.float32)
    inv_rms = lax.rsqrt(jnp.mean(x_f32 * x_f32, axis=-1, keepdims=True) + 1e-5)
    return (x_f32 * inv_rms * norm_gain.astype(jnp.float32)).astype(jnp.bfloat16)


def rotary_tables(positions, head_dim):
    half_dim = head_dim // 2
    inv_freq = 10000.0 ** (-2.0 * jnp.arange(half_dim, dtype=jnp.float32) / head_dim)
    angles = positions.astype(jnp.float32)[:, :, None] * inv_freq
    cos_part, sin_part = jnp.cos(angles), jnp.sin(angles)
    cos_tab = jnp.concatenate([cos_part, cos_part], axis=-1)
    sin_tab = jnp.concatenate([-sin_part, sin_part], axis=-1)
    return cos_tab.reshape(-1, head_dim), sin_tab.reshape(-1, head_dim)


def group_barrier(me, n_cp):
    barrier = pltpu.get_barrier_semaphore()

    def signal(k, _):
        pl.semaphore_signal(barrier, inc=1, device_id={AXIS: lax.rem(me + k, n_cp)}, device_id_type=pl.DeviceIdType.MESH)
        return 0

    lax.fori_loop(1, n_cp, signal, 0)
    pl.semaphore_wait(barrier, n_cp - 1)


def put(src, dst, owner, me, send_sem, recv_sem):
    @pl.when(owner == me)
    def _():
        pltpu.make_async_copy(src, dst, recv_sem).start()

    @pl.when(owner != me)
    def _():
        pltpu.make_async_remote_copy(src, dst, send_sem, recv_sem, device_id={AXIS: owner}, device_id_type=pl.DeviceIdType.MESH).start()


def wait_bytes_of(ref, sem):
    pltpu.make_async_copy(ref, ref, sem).wait()


def project_kernel(n_cp, n_kv, per_dev, h_ref, cos_ref, sin_ref, wq_ref, wk_ref, wv_ref, q_out, kv_out, w_buf, acc, stage, w_sem, send_sem, recv_q, recv_kv):
    me = lax.axis_index(AXIS)
    chip = me // 2
    n_steps, batch, seq, width = stage.shape
    head_dim = width // 2
    half_dim = head_dim // 2
    n_q = n_steps - n_kv

    def kv_block(step):
        return lax.rem(step + chip, n_kv)

    def q_block(step):
        return lax.rem(step - n_kv + chip, n_q)

    def fetch(step, slot):
        @pl.when(step < n_kv)
        def _():
            cols = pl.ds(pl.multiple_of(kv_block(step) * head_dim, head_dim), head_dim)
            pltpu.make_async_copy(wk_ref.at[:, cols], w_buf.at[slot, :, pl.ds(0, head_dim)], w_sem.at[slot]).start()
            pltpu.make_async_copy(wv_ref.at[:, cols], w_buf.at[slot, :, pl.ds(head_dim, head_dim)], w_sem.at[slot]).start()

        @pl.when(step >= n_kv)
        def _():
            cols = pl.ds(pl.multiple_of(q_block(step) * width, width), width)
            pltpu.make_async_copy(wq_ref.at[:, cols], w_buf.at[slot], w_sem.at[slot]).start()

    def send(step):
        @pl.when(step < n_kv)
        def _():
            head = kv_block(step)
            for b in range(batch):
                pair = b * n_kv + head
                first, second = (2 * pair) // per_dev, (2 * pair + 1) // per_dev
                src = stage.at[step, b]
                rows = pl.ds(me * seq, seq)
                put(src, kv_out.at[pair - (per_dev * first) // 2, rows], first, me, send_sem, recv_kv)

                @pl.when(second != first)
                def _():
                    put(src, kv_out.at[pair - (per_dev * second) // 2, rows], second, me, send_sem, recv_kv)

        @pl.when(step >= n_kv)
        def _():
            head = q_block(step)
            for b in range(batch):
                unit = b * n_q + head
                owner = unit // per_dev
                put(stage.at[step, b], q_out.at[unit - per_dev * owner, pl.ds(me * seq, seq)], owner, me, send_sem, recv_q)

    fetch(0, 0)
    group_barrier(me, n_cp)

    def rotate(x):
        return (x * cos_ref[...] + pltpu.roll(x, half_dim, 1) * sin_ref[...]).astype(jnp.bfloat16).reshape(batch, seq, head_dim)

    def body(step, _):
        slot = lax.rem(step, 2)
        wait_bytes_of(w_buf.at[slot], w_sem.at[slot])

        @pl.when(step + 1 < n_steps)
        def _():
            fetch(step + 1, 1 - slot)

        acc[...] = jnp.dot(h_ref[...], w_buf[slot], preferred_element_type=jnp.float32)
        stage[step, :, :, 0:head_dim] = rotate(acc[:, 0:head_dim])

        @pl.when(step < n_kv)
        def _():
            stage[step, :, :, head_dim:width] = acc[:, head_dim:width].astype(jnp.bfloat16).reshape(batch, seq, head_dim)

        @pl.when(step >= n_kv)
        def _():
            stage[step, :, :, head_dim:width] = rotate(acc[:, head_dim:width])

        @pl.when(step > 0)
        def _():
            send(step - 1)

        return 0

    lax.fori_loop(0, n_steps, body, 0)
    send(n_steps - 1)
    away = (n_cp - 1) * seq
    wait_bytes_of(q_out.at[:, pl.ds(0, away)], send_sem)
    wait_bytes_of(kv_out.at[:, pl.ds(0, away)], send_sem)
    wait_bytes_of(q_out, recv_q)
    wait_bytes_of(kv_out, recv_kv)


def attend_kernel(n_cp, per_dev, blk_q, blk_k, q_ref, kv_ref, o_out, v_t, stage, acc, send_sem, recv_sem):
    me = lax.axis_index(AXIS)
    n_units, total, width = q_ref.shape
    head_dim = width // 2
    batch, seq, model = o_out.shape
    n_q = model // width
    n_blocks = total // blk_q
    span = blk_q // seq
    factor = LOG2E * head_dim ** -0.5

    group_barrier(me, n_cp)
    for s in range(kv_ref.shape[0]):
        def turn(c, _):
            rows = pl.ds(pl.multiple_of(c * blk_k, blk_k), blk_k)
            v_t[s, :, rows] = kv_ref[s, rows, head_dim:width].astype(jnp.float32).T.astype(jnp.bfloat16)
            return 0

        lax.fori_loop(0, total // blk_k, turn, 0)

    def block_of(t):
        return lax.rem(t + me // 2 + 1, n_blocks)

    def send(t):
        unit, i = t // n_blocks, block_of(lax.rem(t, n_blocks))
        half = per_dev * me + unit
        b = half // n_q
        cols = pl.ds(pl.multiple_of(lax.rem(half, n_q) * width, width), width)
        for r in range(span):
            owner = i * span + r
            put(stage.at[unit, pl.ds(owner * seq, seq)], o_out.at[b, :, cols], owner, me, send_sem, recv_sem)

    def scores(kv_slot, start, size, q_head):
        k_blk = kv_ref[kv_slot, pl.ds(pl.multiple_of(start, blk_q), size), 0:head_dim]
        return lax.dot_general(k_blk, q_head, (((1,), (1,)), ((), ())), preferred_element_type=jnp.float32)

    def weigh(kv_slot, start, size, prob):
        return jnp.dot(v_t[kv_slot, :, pl.ds(pl.multiple_of(start, blk_q), size)], prob.astype(jnp.bfloat16), preferred_element_type=jnp.float32)

    def step(t, _):
        unit, i = t // n_blocks, block_of(lax.rem(t, n_blocks))
        kv_slot = (per_dev * me + unit) // 2 - (per_dev * me) // 2
        q_start = pl.multiple_of(i * blk_q, blk_q)
        q_rows = pl.ds(q_start, blk_q)
        q_heads = [q_ref[unit, q_rows, g * head_dim:(g + 1) * head_dim] for g in range(2)]

        def diagonal(size):
            start = q_start + blk_q - size
            allowed = lax.broadcasted_iota(jnp.int32, (size, blk_q), 0) - (size - blk_q) <= lax.broadcasted_iota(jnp.int32, (size, blk_q), 1)
            out = []
            for g in range(2):
                s = jnp.where(allowed, scores(kv_slot, start, size, q_heads[g]), -jnp.inf)
                top = jnp.max(s, axis=0, keepdims=True)
                prob = jnp.exp2(s * factor - top * factor)
                acc[g] = weigh(kv_slot, start, size, prob)
                out += [top, jnp.sum(prob, axis=0, keepdims=True)]
            return tuple(out)

        state = lax.cond(lax.rem(i, 2) == 0, lambda: diagonal(blk_q), lambda: diagonal(2 * blk_q))

        def full(j, state):
            start = j * blk_k
            all_s = [scores(kv_slot, start, blk_k, q_heads[g]) for g in range(2)]
            out = []
            for g in range(2):
                top, total_p = state[2 * g], state[2 * g + 1]
                s = all_s[g]
                new_top = jnp.maximum(top, jnp.max(s, axis=0, keepdims=True))
                prob = jnp.exp2(s * factor - new_top * factor)
                rescale = jnp.exp2(top * factor - new_top * factor)
                acc[g] = acc[g] * rescale + weigh(kv_slot, start, blk_k, prob)
                out += [new_top, total_p * rescale + jnp.sum(prob, axis=0, keepdims=True)]
            return tuple(out)

        state = lax.fori_loop(0, i // 2, full, state)
        for g in range(2):
            stage[unit, q_rows, g * head_dim:(g + 1) * head_dim] = (acc[g] / state[2 * g + 1]).T.astype(jnp.bfloat16)

        @pl.when(t > 0)
        def _():
            send(t - 1)

        return 0

    n_all = n_units * n_blocks
    lax.fori_loop(0, n_all, step, 0)
    send(n_all - 1)
    wait_bytes_of(stage.at[:, pl.ds(0, total - seq)], send_sem)
    wait_bytes_of(o_out, recv_sem)


def solution(mesh):
    n_cp = mesh.shape[AXIS]

    def local_block(hidden, positions, norm_gain, w_query, w_key, w_value, w_out):
        batch, seq, model_dim = hidden.shape
        n_heads, head_dim, _ = w_out.shape
        n_kv = w_key.shape[1] // head_dim
        width = 2 * head_dim
        n_q = n_heads // 2
        per_dev = batch * n_q // n_cp
        n_slots = per_dev // 2 + 1
        total = n_cp * seq
        n_steps = n_kv + n_q
        any_space = pl.BlockSpec(memory_space=pl.ANY)
        vmem = pl.BlockSpec(memory_space=pltpu.VMEM)
        normed = rms_norm(hidden, norm_gain).reshape(batch * seq, model_dim)
        cos_tab, sin_tab = rotary_tables(positions, head_dim)
        q_all, kv_all = pl.pallas_call(
            functools.partial(project_kernel, n_cp, n_kv, per_dev),
            out_shape=(
                jax.ShapeDtypeStruct((per_dev, total, width), jnp.bfloat16),
                jax.ShapeDtypeStruct((n_slots, total, width), jnp.bfloat16),
            ),
            in_specs=[vmem, vmem, vmem, any_space, any_space, any_space],
            out_specs=(any_space, any_space),
            scratch_shapes=[
                pltpu.VMEM((2, model_dim, width), jnp.bfloat16),
                pltpu.VMEM((batch * seq, width), jnp.float32),
                pltpu.VMEM((n_steps, batch, seq, width), jnp.bfloat16),
                pltpu.SemaphoreType.DMA((2,)),
                pltpu.SemaphoreType.DMA,
                pltpu.SemaphoreType.DMA,
                pltpu.SemaphoreType.DMA,
            ],
            compiler_params=pltpu.CompilerParams(collective_id=0, has_side_effects=True, vmem_limit_bytes=VMEM_LIMIT),
            name='project_and_send',
        )(normed, cos_tab, sin_tab, w_query, w_key, w_value)
        blk_q = 2 * seq
        attn_out = pl.pallas_call(
            functools.partial(attend_kernel, n_cp, per_dev, blk_q, 2 * blk_q),
            out_shape=jax.ShapeDtypeStruct((batch, seq, n_heads * head_dim), jnp.bfloat16),
            in_specs=[vmem, vmem],
            out_specs=any_space,
            scratch_shapes=[
                pltpu.VMEM((n_slots, head_dim, total), jnp.bfloat16),
                pltpu.VMEM((per_dev, total, width), jnp.bfloat16),
                pltpu.VMEM((2, head_dim, blk_q), jnp.float32),
                pltpu.SemaphoreType.DMA,
                pltpu.SemaphoreType.DMA,
            ],
            compiler_params=pltpu.CompilerParams(collective_id=1, has_side_effects=True, vmem_limit_bytes=VMEM_LIMIT),
            name='attend_and_return',
        )(q_all, kv_all)
        proj_out = jnp.einsum('bqe,ed->bqd', attn_out, w_out.reshape(n_heads * head_dim, model_dim), preferred_element_type=jnp.float32)
        return (hidden.astype(jnp.float32) + proj_out).astype(jnp.bfloat16)

    act_spec = P('dp', 'cp', None)
    return jax.shard_map(local_block, mesh=mesh, in_specs=(act_spec, P('dp', 'cp'), P(), P(), P(), P(), P()), out_specs=act_spec, check_vma=False)
```

```python
import functools

import jax
import jax.numpy as jnp
from jax import lax
from jax.experimental import pallas as pl
from jax.experimental.pallas import tpu as pltpu
from jax.sharding import PartitionSpec as P

AXIS = 'cp'
LOG2E = 1.4426950408889634
CHUNK = 32
VMEM_LIMIT = 60 * 1024 * 1024


def rms_norm(hidden, norm_gain):
    x_f32 = hidden.astype(jnp.float32)
    inv_rms = lax.rsqrt(jnp.mean(x_f32 * x_f32, axis=-1, keepdims=True) + 1e-5)
    return (x_f32 * inv_rms * norm_gain.astype(jnp.float32)).astype(jnp.bfloat16)


def rotary_tables(positions, head_dim):
    half_dim = head_dim // 2
    inv_freq = 10000.0 ** (-2.0 * jnp.arange(half_dim, dtype=jnp.float32) / head_dim)
    angles = positions.astype(jnp.float32)[:, :, None] * inv_freq
    cos_part, sin_part = jnp.cos(angles), jnp.sin(angles)
    cos_tab = jnp.concatenate([cos_part, cos_part], axis=-1)
    sin_tab = jnp.concatenate([-sin_part, sin_part], axis=-1)
    return cos_tab.reshape(-1, head_dim), sin_tab.reshape(-1, head_dim)


def group_barrier(me, n_cp):
    barrier = pltpu.get_barrier_semaphore()

    def signal(k, _):
        pl.semaphore_signal(barrier, inc=1, device_id={AXIS: lax.rem(me + k, n_cp)}, device_id_type=pl.DeviceIdType.MESH)
        return 0

    lax.fori_loop(1, n_cp, signal, 0)
    pl.semaphore_wait(barrier, n_cp - 1)


def put(src, dst, owner, me, send_sem, recv_sem):
    @pl.when(owner == me)
    def _():
        pltpu.make_async_copy(src, dst, recv_sem).start()

    @pl.when(owner != me)
    def _():
        pltpu.make_async_remote_copy(src, dst, send_sem, recv_sem, device_id={AXIS: owner}, device_id_type=pl.DeviceIdType.MESH).start()


def wait_bytes_of(ref, sem):
    pltpu.make_async_copy(ref, ref, sem).wait()


def project_kernel(n_cp, n_kv, per_dev, h_ref, cos_ref, sin_ref, wq_ref, wk_ref, wv_ref, q_out, kv_out, w_buf, acc, stage, w_sem, send_sem, recv_q, recv_kv):
    me = lax.axis_index(AXIS)
    chip = me // 2
    n_steps, batch, seq, width = stage.shape
    head_dim = width // 2
    half_dim = head_dim // 2
    n_q = n_steps - n_kv

    def kv_block(step):
        return lax.rem(step + chip, n_kv)

    def q_block(step):
        return lax.rem(step - n_kv + chip, n_q)

    def fetch(step, slot):
        @pl.when(step < n_kv)
        def _():
            cols = pl.ds(pl.multiple_of(kv_block(step) * head_dim, head_dim), head_dim)
            pltpu.make_async_copy(wk_ref.at[:, cols], w_buf.at[slot, :, pl.ds(0, head_dim)], w_sem.at[slot]).start()
            pltpu.make_async_copy(wv_ref.at[:, cols], w_buf.at[slot, :, pl.ds(head_dim, head_dim)], w_sem.at[slot]).start()

        @pl.when(step >= n_kv)
        def _():
            cols = pl.ds(pl.multiple_of(q_block(step) * width, width), width)
            pltpu.make_async_copy(wq_ref.at[:, cols], w_buf.at[slot], w_sem.at[slot]).start()

    def send(step):
        @pl.when(step < n_kv)
        def _():
            head = kv_block(step)
            for b in range(batch):
                pair = b * n_kv + head
                first, second = (2 * pair) // per_dev, (2 * pair + 1) // per_dev
                src = stage.at[step, b]
                rows = pl.ds(me * seq, seq)
                put(src, kv_out.at[pair - (per_dev * first) // 2, rows], first, me, send_sem, recv_kv)

                @pl.when(second != first)
                def _():
                    put(src, kv_out.at[pair - (per_dev * second) // 2, rows], second, me, send_sem, recv_kv)

        @pl.when(step >= n_kv)
        def _():
            head = q_block(step)
            for b in range(batch):
                unit = b * n_q + head
                owner = unit // per_dev
                put(stage.at[step, b], q_out.at[unit - per_dev * owner, pl.ds(me * seq, seq)], owner, me, send_sem, recv_q)

    fetch(0, 0)
    group_barrier(me, n_cp)

    def rotate(x):
        return (x * cos_ref[...] + pltpu.roll(x, half_dim, 1) * sin_ref[...]).astype(jnp.bfloat16).reshape(batch, seq, head_dim)

    def body(step, _):
        slot = lax.rem(step, 2)
        wait_bytes_of(w_buf.at[slot], w_sem.at[slot])

        @pl.when(step + 1 < n_steps)
        def _():
            fetch(step + 1, 1 - slot)

        acc[...] = jnp.dot(h_ref[...], w_buf[slot], preferred_element_type=jnp.float32)
        stage[step, :, :, 0:head_dim] = rotate(acc[:, 0:head_dim])

        @pl.when(step < n_kv)
        def _():
            stage[step, :, :, head_dim:width] = acc[:, head_dim:width].astype(jnp.bfloat16).reshape(batch, seq, head_dim)

        @pl.when(step >= n_kv)
        def _():
            stage[step, :, :, head_dim:width] = rotate(acc[:, head_dim:width])

        @pl.when(step > 0)
        def _():
            send(step - 1)

        return 0

    lax.fori_loop(0, n_steps, body, 0)
    send(n_steps - 1)
    away = (n_cp - 1) * seq
    wait_bytes_of(q_out.at[:, pl.ds(0, away)], send_sem)
    wait_bytes_of(kv_out.at[:, pl.ds(0, away)], send_sem)
    wait_bytes_of(q_out, recv_q)
    wait_bytes_of(kv_out, recv_kv)


def attend_kernel(n_cp, per_dev, blk_q, blk_k, q_ref, kv_ref, o_out, v_t, stage, s_buf, p_buf, acc, stat, send_sem, recv_sem):
    me = lax.axis_index(AXIS)
    n_units, total, width = q_ref.shape
    head_dim = width // 2
    batch, seq, model = o_out.shape
    n_q = model // width
    n_blocks = total // blk_q
    n_all = n_units * n_blocks
    ratio = blk_k // blk_q
    span = blk_q // seq
    factor = LOG2E * head_dim ** -0.5

    group_barrier(me, n_cp)
    for s in range(kv_ref.shape[0]):
        def turn(c, _):
            rows = pl.ds(pl.multiple_of(c * blk_k, blk_k), blk_k)
            v_t[s, :, rows] = kv_ref[s, rows, head_dim:width].astype(jnp.float32).T.astype(jnp.bfloat16)
            return 0

        lax.fori_loop(0, total // blk_k, turn, 0)

    def place(t):
        unit = t // n_blocks
        i = lax.rem(lax.rem(t, n_blocks) + me // 2 + 1, n_blocks)
        slot = (per_dev * me + unit) // 2 - (per_dev * me) // 2
        return unit, slot, i, i // ratio

    def send(t):
        unit, _, i, _ = place(t)
        half = per_dev * me + unit
        b = half // n_q
        cols = pl.ds(pl.multiple_of(lax.rem(half, n_q) * width, width), width)
        for r in range(span):
            owner = i * span + r
            put(stage.at[unit, pl.ds(owner * seq, seq)], o_out.at[b, :, cols], owner, me, send_sem, recv_sem)

    def next_scores(unit, slot, i, j):
        k_blk = kv_ref[slot, pl.ds(pl.multiple_of(j * blk_k, blk_k), blk_k), 0:head_dim]
        q_rows = pl.ds(pl.multiple_of(i * blk_q, blk_q), blk_q)
        for g in range(2):
            q_head = q_ref[unit, q_rows, g * head_dim:(g + 1) * head_dim]
            cols = slice(g * blk_q, (g + 1) * blk_q)
            s = lax.dot_general(k_blk, q_head, (((1,), (1,)), ((), ())), preferred_element_type=jnp.float32)
            s_buf[:, cols] = s
            stat[3, 0:1, cols] = jnp.max(s, axis=0, keepdims=True)

    def weighed(slot, j):
        cols = pl.ds(pl.multiple_of(j * blk_k, blk_k), blk_k)
        return acc[...] * stat[2, 0:1, :] + jnp.dot(v_t[slot, :, cols], p_buf[...], preferred_element_type=jnp.float32)

    def finish(t):
        unit, slot, i, n_full = place(t)
        out = weighed(slot, jnp.maximum(n_full - 1, 0)) * (1.0 / stat[1, 0:1, :])
        q_rows = pl.ds(pl.multiple_of(i * blk_q, blk_q), blk_q)
        for g in range(2):
            stage[unit, q_rows, g * head_dim:(g + 1) * head_dim] = out[:, g * blk_q:(g + 1) * blk_q].T.astype(jnp.bfloat16)

    def step(t, _):
        unit, slot, i, n_full = place(t)
        after = place(jnp.minimum(t + 1, n_all - 1))

        def follow(j, n_done):
            more = n_done < n_full
            pick = lambda here, there: jnp.where(more, here, there)
            next_scores(pick(unit, after[0]), pick(slot, after[1]), pick(i, after[2]), pick(n_done, after[3]))

        @pl.when(t > 1)
        def _():
            send(t - 2)

        def diagonal(size):
            finish(jnp.maximum(t - 1, 0))
            acc[...] = jnp.zeros_like(acc)
            shape = (size, 2 * blk_q)
            allowed = lax.broadcasted_iota(jnp.int32, shape, 0) - (size - blk_q) <= lax.rem(lax.broadcasted_iota(jnp.int32, shape, 1), blk_q)
            s = jnp.where(allowed, s_buf[0:size, :], -jnp.inf)
            top = jnp.max(s, axis=0, keepdims=True)
            prob = jnp.exp2(s * factor - top * factor)
            stat[0, 0:1, :] = top
            stat[1, 0:1, :] = jnp.sum(prob, axis=0, keepdims=True)
            stat[2, 0:1, :] = jnp.ones_like(top)
            p_buf[0:size, :] = prob.astype(jnp.bfloat16)
            if size < blk_k:
                p_buf[size:blk_k, :] = jnp.zeros((blk_k - size, 2 * blk_q), jnp.bfloat16)
            follow(None, 0)

        for r in range(ratio):
            pl.when(lax.rem(i, ratio) == r)(functools.partial(diagonal, (r + 1) * blk_q))

        def full(j, _):
            acc[...] = weighed(slot, jnp.where(j == 0, n_full, j - 1))
            top = stat[0, 0:1, :]
            new_top = jnp.maximum(top, stat[3, 0:1, :])
            shift = new_top * factor
            rescale = jnp.exp2(top * factor - shift)
            part = jnp.zeros((8, 2 * blk_q), jnp.float32)
            for r in range(0, blk_k, CHUNK):
                prob = jnp.exp2(s_buf[r:r + CHUNK, :] * factor - shift)
                part = part + jnp.sum(prob.reshape(CHUNK // 8, 8, 2 * blk_q), axis=0)
                p_buf[r:r + CHUNK, :] = prob.astype(jnp.bfloat16)
            stat[0, 0:1, :] = new_top
            stat[1, 0:1, :] = stat[1, 0:1, :] * rescale + jnp.sum(part, axis=0, keepdims=True)
            stat[2, 0:1, :] = rescale
            follow(j, j + 1)
            return 0

        lax.fori_loop(0, n_full, full, 0)
        return 0

    acc[...] = jnp.zeros_like(acc)
    stat[...] = jnp.ones_like(stat)
    p_buf[...] = jnp.zeros_like(p_buf)
    first = place(0)
    next_scores(first[0], first[1], first[2], first[3])
    lax.fori_loop(0, n_all, step, 0)
    send(n_all - 2)
    finish(n_all - 1)
    send(n_all - 1)
    wait_bytes_of(stage.at[:, pl.ds(0, total - seq)], send_sem)
    wait_bytes_of(o_out, recv_sem)


def solution(mesh):
    n_cp = mesh.shape[AXIS]

    def local_block(hidden, positions, norm_gain, w_query, w_key, w_value, w_out):
        batch, seq, model_dim = hidden.shape
        n_heads, head_dim, _ = w_out.shape
        n_kv = w_key.shape[1] // head_dim
        width = 2 * head_dim
        n_q = n_heads // 2
        per_dev = batch * n_q // n_cp
        n_slots = per_dev // 2 + 1
        total = n_cp * seq
        n_steps = n_kv + n_q
        any_space = pl.BlockSpec(memory_space=pl.ANY)
        vmem = pl.BlockSpec(memory_space=pltpu.VMEM)
        normed = rms_norm(hidden, norm_gain).reshape(batch * seq, model_dim)
        cos_tab, sin_tab = rotary_tables(positions, head_dim)
        q_all, kv_all = pl.pallas_call(
            functools.partial(project_kernel, n_cp, n_kv, per_dev),
            out_shape=(
                jax.ShapeDtypeStruct((per_dev, total, width), jnp.bfloat16),
                jax.ShapeDtypeStruct((n_slots, total, width), jnp.bfloat16),
            ),
            in_specs=[vmem, vmem, vmem, any_space, any_space, any_space],
            out_specs=(any_space, any_space),
            scratch_shapes=[
                pltpu.VMEM((2, model_dim, width), jnp.bfloat16),
                pltpu.VMEM((batch * seq, width), jnp.float32),
                pltpu.VMEM((n_steps, batch, seq, width), jnp.bfloat16),
                pltpu.SemaphoreType.DMA((2,)),
                pltpu.SemaphoreType.DMA,
                pltpu.SemaphoreType.DMA,
                pltpu.SemaphoreType.DMA,
            ],
            compiler_params=pltpu.CompilerParams(collective_id=0, has_side_effects=True, vmem_limit_bytes=VMEM_LIMIT),
            name='project_and_send',
        )(normed, cos_tab, sin_tab, w_query, w_key, w_value)
        blk_q = 2 * seq
        attn_out = pl.pallas_call(
            functools.partial(attend_kernel, n_cp, per_dev, blk_q, 2 * blk_q),
            out_shape=jax.ShapeDtypeStruct((batch, seq, n_heads * head_dim), jnp.bfloat16),
            in_specs=[vmem, vmem],
            out_specs=any_space,
            scratch_shapes=[
                pltpu.VMEM((n_slots, head_dim, total), jnp.bfloat16),
                pltpu.VMEM((per_dev, total, width), jnp.bfloat16),
                pltpu.VMEM((2 * blk_q, 2 * blk_q), jnp.float32),
                pltpu.VMEM((2 * blk_q, 2 * blk_q), jnp.bfloat16),
                pltpu.VMEM((head_dim, 2 * blk_q), jnp.float32),
                pltpu.VMEM((4, 8, 2 * blk_q), jnp.float32),
                pltpu.SemaphoreType.DMA,
                pltpu.SemaphoreType.DMA,
            ],
            compiler_params=pltpu.CompilerParams(collective_id=1, has_side_effects=True, vmem_limit_bytes=VMEM_LIMIT),
            name='attend_and_return',
        )(q_all, kv_all)
        proj_out = jnp.einsum('bqe,ed->bqd', attn_out, w_out.reshape(n_heads * head_dim, model_dim), preferred_element_type=jnp.float32)
        return (hidden.astype(jnp.float32) + proj_out).astype(jnp.bfloat16)

    act_spec = P('dp', 'cp', None)
    return jax.shard_map(local_block, mesh=mesh, in_specs=(act_spec, P('dp', 'cp'), P(), P(), P(), P(), P()), out_specs=act_spec, check_vma=False)
```

```python
import functools

import jax
import jax.numpy as jnp
from jax import lax
from jax.experimental import pallas as pl
from jax.experimental.pallas import tpu as pltpu
from jax.sharding import PartitionSpec as P

AXIS = 'cp'
LOG2E = 1.4426950408889634
CHUNK = 32
VMEM_LIMIT = 60 * 1024 * 1024


def rms_norm(hidden, norm_gain):
    x_f32 = hidden.astype(jnp.float32)
    inv_rms = lax.rsqrt(jnp.mean(x_f32 * x_f32, axis=-1, keepdims=True) + 1e-5)
    return (x_f32 * inv_rms * norm_gain.astype(jnp.float32)).astype(jnp.bfloat16)


def rotary_tables(positions, head_dim):
    half_dim = head_dim // 2
    inv_freq = 10000.0 ** (-2.0 * jnp.arange(half_dim, dtype=jnp.float32) / head_dim)
    angles = positions.astype(jnp.float32)[:, :, None] * inv_freq
    cos_part, sin_part = jnp.cos(angles), jnp.sin(angles)
    cos_tab = jnp.concatenate([cos_part, cos_part], axis=-1)
    sin_tab = jnp.concatenate([-sin_part, sin_part], axis=-1)
    return cos_tab.reshape(-1, head_dim), sin_tab.reshape(-1, head_dim)


def group_barrier(me, n_cp):
    barrier = pltpu.get_barrier_semaphore()

    def signal(k, _):
        pl.semaphore_signal(barrier, inc=1, device_id={AXIS: lax.rem(me + k, n_cp)}, device_id_type=pl.DeviceIdType.MESH)
        return 0

    lax.fori_loop(1, n_cp, signal, 0)
    pl.semaphore_wait(barrier, n_cp - 1)


def put(src, dst, owner, me, send_sem, recv_sem):
    @pl.when(owner == me)
    def _():
        pltpu.make_async_copy(src, dst, recv_sem).start()

    @pl.when(owner != me)
    def _():
        pltpu.make_async_remote_copy(src, dst, send_sem, recv_sem, device_id={AXIS: owner}, device_id_type=pl.DeviceIdType.MESH).start()


def wait_bytes_of(ref, sem):
    pltpu.make_async_copy(ref, ref, sem).wait()


def block_kernel(
    n_cp, h_ref, cos_ref, sin_ref, wq_ref, wk_ref, wv_ref, wo_ref, x_ref, y_ref,
    w_buf, acc, stage, q_in, kv_in, v_t, o_stage, s_buf, p_buf, o_acc, stat, o_in, x_buf, y_buf,
    w_sem, x_sem, y_sem, send_q, send_kv, send_o, send_half, recv_q, recv_kv, recv_o, recv_half,
):
    me = lax.axis_index(AXIS)
    chip, core = me // 2, lax.rem(me, 2)
    n_steps, batch, seq, width = stage.shape
    rounds, total, _ = q_in.shape
    per_round = batch // rounds
    n_q = n_cp // per_round
    n_kv = n_steps - n_q
    head_dim = width // 2
    half_dim = head_dim // 2
    blk_q = s_buf.shape[1] // 2
    blk_k = s_buf.shape[0]
    n_blocks = total // blk_q
    ratio = blk_k // blk_q
    span = blk_q // seq
    chips_per_k = blk_k // (2 * seq)
    factor = LOG2E * head_dim ** -0.5

    def kv_block(step):
        return lax.rem(step + chip, n_kv)

    def q_block(step):
        return lax.rem(step - n_kv + chip, n_q)

    def fetch(step, slot):
        @pl.when(step < n_kv)
        def _():
            cols = pl.ds(pl.multiple_of(kv_block(step) * head_dim, head_dim), head_dim)
            pltpu.make_async_copy(wk_ref.at[:, cols], w_buf.at[slot, :, pl.ds(0, head_dim)], w_sem.at[slot]).start()
            pltpu.make_async_copy(wv_ref.at[:, cols], w_buf.at[slot, :, pl.ds(head_dim, head_dim)], w_sem.at[slot]).start()

        @pl.when(step >= n_kv)
        def _():
            cols = pl.ds(pl.multiple_of(q_block(step) * width, width), width)
            pltpu.make_async_copy(wq_ref.at[:, cols], w_buf.at[slot], w_sem.at[slot]).start()

    def send_kv_tiles(step):
        for b in range(batch):
            owner = 2 * (b % per_round * n_kv + kv_block(step)) + core
            r = b // per_round
            put(stage.at[step, b], kv_in.at[r, chip, core], owner, me, send_kv, recv_kv.at[r])

    def send_q_tiles(step, r):
        for k in range(per_round):
            put(stage.at[step, r * per_round + k], q_in.at[r, pl.ds(me * seq, seq)], k * n_q + q_block(step), me, send_q, recv_q.at[r])

    def send_first(step):
        @pl.when(step < n_kv)
        def _():
            send_kv_tiles(step)

        @pl.when(step >= n_kv)
        def _():
            send_q_tiles(step, 0)

    fetch(0, 0)
    group_barrier(me, n_cp)

    def rotate(x):
        return (x * cos_ref[...] + pltpu.roll(x, half_dim, 1) * sin_ref[...]).astype(jnp.bfloat16).reshape(batch, seq, head_dim)

    def project(step, _):
        slot = lax.rem(step, 2)
        wait_bytes_of(w_buf.at[slot], w_sem.at[slot])

        @pl.when(step + 1 < n_steps)
        def _():
            fetch(step + 1, 1 - slot)

        acc[...] = jnp.dot(h_ref[...], w_buf[slot], preferred_element_type=jnp.float32)
        stage[step, :, :, 0:head_dim] = rotate(acc[:, 0:head_dim])

        @pl.when(step < n_kv)
        def _():
            stage[step, :, :, head_dim:width] = acc[:, head_dim:width].astype(jnp.bfloat16).reshape(batch, seq, head_dim)

        @pl.when(step >= n_kv)
        def _():
            stage[step, :, :, head_dim:width] = rotate(acc[:, head_dim:width])

        @pl.when(step > 0)
        def _():
            send_first(step - 1)

        return 0

    lax.fori_loop(0, n_steps, project, 0)
    send_first(n_steps - 1)

    def send_rest(k, _):
        send_q_tiles(n_kv + lax.rem(k, n_q), 1 + k // n_q)
        return 0

    lax.fori_loop(0, (rounds - 1) * n_q, send_rest, 0)

    def out_fetch(k, slot):
        r, cols = k // n_out, pl.ds(pl.multiple_of(lax.rem(k, n_out) * width, width), width)
        pltpu.make_async_copy(wo_ref.at[:, cols], w_buf.at[slot], w_sem.at[slot]).start()
        pltpu.make_async_copy(x_ref.at[pl.ds(r * per_round, per_round), :, cols], x_buf.at[slot], x_sem.at[slot]).start()

    n_out = wo_ref.shape[1] // width
    out_fetch(0, 0)

    def place(t):
        i = lax.rem(t + chip + 1, n_blocks)
        return i, i // ratio

    def attend(r, _):
        wait_bytes_of(kv_in.at[r, :, 0], recv_kv.at[r])
        mine = kv_in.at[r, :, core]
        pltpu.make_async_remote_copy(mine, mine, send_half, recv_half.at[r], device_id={AXIS: me + 1 - 2 * core}, device_id_type=pl.DeviceIdType.MESH).start()
        wait_bytes_of(q_in.at[r], recv_q.at[r])
        wait_bytes_of(kv_in.at[r, :, 0], recv_half.at[r])

        def kv_rows(j, lanes):
            return kv_in[r, pl.ds(j * chips_per_k, chips_per_k), :, :, lanes].reshape(blk_k, head_dim)

        def turn(j, _):
            v_t[:, pl.ds(pl.multiple_of(j * blk_k, blk_k), blk_k)] = kv_rows(j, slice(head_dim, width)).astype(jnp.float32).T.astype(jnp.bfloat16)
            return 0

        lax.fori_loop(0, total // blk_k, turn, 0)

        def send(t):
            i, _ = place(t)
            b = r * per_round + me // n_q
            cols = pl.ds(pl.multiple_of(lax.rem(me, n_q) * width, width), width)
            for s in range(span):
                owner = i * span + s
                put(o_stage.at[r, pl.ds(owner * seq, seq)], o_in.at[b, :, cols], owner, me, send_o, recv_o.at[r])

        def next_scores(i, j):
            k_blk = kv_rows(j, slice(0, head_dim))
            q_rows = pl.ds(pl.multiple_of(i * blk_q, blk_q), blk_q)
            for g in range(2):
                q_head = q_in[r, q_rows, g * head_dim:(g + 1) * head_dim]
                cols = slice(g * blk_q, (g + 1) * blk_q)
                s = lax.dot_general(k_blk, q_head, (((1,), (1,)), ((), ())), preferred_element_type=jnp.float32)
                s_buf[:, cols] = s
                stat[3, 0:1, cols] = jnp.max(s, axis=0, keepdims=True)

        def weighed(j):
            cols = pl.ds(pl.multiple_of(j * blk_k, blk_k), blk_k)
            return o_acc[...] * stat[2, 0:1, :] + jnp.dot(v_t[:, cols], p_buf[...], preferred_element_type=jnp.float32)

        def finish(t):
            i, n_full = place(t)
            out = weighed(jnp.maximum(n_full - 1, 0)) * (1.0 / stat[1, 0:1, :])
            q_rows = pl.ds(pl.multiple_of(i * blk_q, blk_q), blk_q)
            for g in range(2):
                o_stage[r, q_rows, g * head_dim:(g + 1) * head_dim] = out[:, g * blk_q:(g + 1) * blk_q].T.astype(jnp.bfloat16)

        def step(t, _):
            i, n_full = place(t)
            after = place(jnp.minimum(t + 1, n_blocks - 1))

            def follow(n_done):
                more = n_done < n_full
                next_scores(jnp.where(more, i, after[0]), jnp.where(more, n_done, after[1]))

            @pl.when(t > 1)
            def _():
                send(t - 2)

            def diagonal(size):
                finish(jnp.maximum(t - 1, 0))
                o_acc[...] = jnp.zeros_like(o_acc)
                shape = (size, 2 * blk_q)
                allowed = lax.broadcasted_iota(jnp.int32, shape, 0) - (size - blk_q) <= lax.rem(lax.broadcasted_iota(jnp.int32, shape, 1), blk_q)
                s = jnp.where(allowed, s_buf[0:size, :], -jnp.inf)
                top = jnp.max(s, axis=0, keepdims=True)
                prob = jnp.exp2(s * factor - top * factor)
                stat[0, 0:1, :] = top
                stat[1, 0:1, :] = jnp.sum(prob, axis=0, keepdims=True)
                stat[2, 0:1, :] = jnp.ones_like(top)
                p_buf[0:size, :] = prob.astype(jnp.bfloat16)
                if size < blk_k:
                    p_buf[size:blk_k, :] = jnp.zeros((blk_k - size, 2 * blk_q), jnp.bfloat16)
                follow(0)

            for part in range(ratio):
                pl.when(lax.rem(i, ratio) == part)(functools.partial(diagonal, (part + 1) * blk_q))

            def full(j, _):
                o_acc[...] = weighed(jnp.where(j == 0, n_full, j - 1))
                top = stat[0, 0:1, :]
                new_top = jnp.maximum(top, stat[3, 0:1, :])
                shift = new_top * factor
                rescale = jnp.exp2(top * factor - shift)
                part_sum = jnp.zeros((8, 2 * blk_q), jnp.float32)
                for k in range(0, blk_k, CHUNK):
                    prob = jnp.exp2(s_buf[k:k + CHUNK, :] * factor - shift)
                    part_sum = part_sum + jnp.sum(prob.reshape(CHUNK // 8, 8, 2 * blk_q), axis=0)
                    p_buf[k:k + CHUNK, :] = prob.astype(jnp.bfloat16)
                stat[0, 0:1, :] = new_top
                stat[1, 0:1, :] = stat[1, 0:1, :] * rescale + jnp.sum(part_sum, axis=0, keepdims=True)
                stat[2, 0:1, :] = rescale
                follow(j + 1)
                return 0

            lax.fori_loop(0, n_full, full, 0)
            return 0

        o_acc[...] = jnp.zeros_like(o_acc)
        stat[...] = jnp.ones_like(stat)
        p_buf[...] = jnp.zeros_like(p_buf)
        next_scores(*place(0))
        lax.fori_loop(0, n_blocks, step, 0)
        send(n_blocks - 2)
        finish(n_blocks - 1)
        send(n_blocks - 1)
        return 0

    lax.fori_loop(0, rounds, attend, 0)

    def y_copy(k, slot):
        r, cols = k // n_out, pl.ds(pl.multiple_of(lax.rem(k, n_out) * width, width), width)
        return pltpu.make_async_copy(y_buf.at[slot], y_ref.at[pl.ds(r * per_round, per_round), :, cols], y_sem.at[slot])

    def out_project(k, _):
        slot, r = lax.rem(k, 2), k // n_out

        @pl.when(k + 1 < rounds * n_out)
        def _():
            out_fetch(k + 1, 1 - slot)

        @pl.when(lax.rem(k, n_out) == 0)
        def _():
            wait_bytes_of(o_in.at[pl.ds(r * per_round, per_round)], recv_o.at[r])

        wait_bytes_of(w_buf.at[slot], w_sem.at[slot])
        wait_bytes_of(x_buf.at[slot], x_sem.at[slot])

        @pl.when(k > 1)
        def _():
            y_copy(k - 2, slot).wait()

        attn = o_in[pl.ds(r * per_round, per_round)].reshape(per_round * seq, wo_ref.shape[0])
        proj = jnp.dot(attn, w_buf[slot], preferred_element_type=jnp.float32)
        y_buf[slot] = (x_buf[slot].astype(jnp.float32) + proj.reshape(per_round, seq, width)).astype(jnp.bfloat16)
        y_copy(k, slot).start()
        return 0

    lax.fori_loop(0, rounds * n_out, out_project, 0)
    for k in (rounds * n_out - 2, rounds * n_out - 1):
        y_copy(k, k % 2).wait()
    away = (n_cp - 1) * seq
    wait_bytes_of(q_in.at[:, pl.ds(0, away)], send_q)
    wait_bytes_of(kv_in.at[:, pl.ds(0, n_cp // 2 - 1), 0], send_kv)
    wait_bytes_of(o_stage.at[:, pl.ds(0, away)], send_o)
    wait_bytes_of(kv_in.at[:, :, 0], send_half)


def solution(mesh):
    n_cp = mesh.shape[AXIS]

    def local_block(hidden, positions, norm_gain, w_query, w_key, w_value, w_out):
        batch, seq, model_dim = hidden.shape
        n_heads, head_dim, _ = w_out.shape
        n_kv = w_key.shape[1] // head_dim
        width = 2 * head_dim
        n_q = n_heads // 2
        rounds = batch * n_q // n_cp
        per_round = batch // rounds
        total = n_cp * seq
        n_steps = n_kv + n_q
        blk_q = 2 * seq
        blk_k = 2 * blk_q
        any_space = pl.BlockSpec(memory_space=pl.ANY)
        vmem = pl.BlockSpec(memory_space=pltpu.VMEM)
        normed = rms_norm(hidden, norm_gain).reshape(batch * seq, model_dim)
        cos_tab, sin_tab = rotary_tables(positions, head_dim)
        dma = pltpu.SemaphoreType.DMA
        return pl.pallas_call(
            functools.partial(block_kernel, n_cp),
            out_shape=jax.ShapeDtypeStruct(hidden.shape, jnp.bfloat16),
            in_specs=[vmem, vmem, vmem] + [any_space] * 5,
            out_specs=any_space,
            scratch_shapes=[
                pltpu.VMEM((2, model_dim, width), jnp.bfloat16),
                pltpu.VMEM((batch * seq, width), jnp.float32),
                pltpu.VMEM((n_steps, batch, seq, width), jnp.bfloat16),
                pltpu.VMEM((rounds, total, width), jnp.bfloat16),
                pltpu.VMEM((rounds, n_cp // 2, 2, seq, width), jnp.bfloat16),
                pltpu.VMEM((head_dim, total), jnp.bfloat16),
                pltpu.VMEM((rounds, total, width), jnp.bfloat16),
                pltpu.VMEM((blk_k, 2 * blk_q), jnp.float32),
                pltpu.VMEM((blk_k, 2 * blk_q), jnp.bfloat16),
                pltpu.VMEM((head_dim, 2 * blk_q), jnp.float32),
                pltpu.VMEM((4, 8, 2 * blk_q), jnp.float32),
                pltpu.VMEM((batch, seq, n_heads * head_dim), jnp.bfloat16),
                pltpu.VMEM((2, per_round, seq, width), jnp.bfloat16),
                pltpu.VMEM((2, per_round, seq, width), jnp.bfloat16),
                dma((2,)), dma((2,)), dma((2,)),
                dma, dma, dma, dma,
                dma((rounds,)), dma((rounds,)), dma((rounds,)), dma((rounds,)),
            ],
            compiler_params=pltpu.CompilerParams(collective_id=0, has_side_effects=True, vmem_limit_bytes=VMEM_LIMIT),
            name='attention_block',
        )(normed, cos_tab, sin_tab, w_query, w_key, w_value, w_out.reshape(n_heads * head_dim, model_dim), hidden)

    act_spec = P('dp', 'cp', None)
    return jax.shard_map(local_block, mesh=mesh, in_specs=(act_spec, P('dp', 'cp'), P(), P(), P(), P(), P()), out_specs=act_spec, check_vma=False)
```

```python
import functools

import jax
import jax.numpy as jnp
from jax import lax
from jax.experimental import pallas as pl
from jax.experimental.pallas import tpu as pltpu
from jax.sharding import PartitionSpec as P

AXIS = 'cp'
LOG2E = 1.4426950408889634
CHUNK = 32
NORM_ROWS = 32
VMEM_LIMIT = 60 * 1024 * 1024


def cos_sin(angles):
    quarter = jnp.round(angles * 0.6366197723675814)
    rest = ((angles - quarter * 1.5703125) - quarter * 4.837512969970703e-4) - quarter * 7.549789954891626e-8
    square = rest * rest
    sin_poly = rest + rest * square * (-1.6666654611e-1 + square * (8.3321608736e-3 - square * 1.9515295891e-4))
    cos_poly = 1.0 - 0.5 * square + square * square * (4.166664568298827e-2 + square * (-1.388731625493765e-3 + square * 2.443315711809948e-5))
    turn = quarter.astype(jnp.int32) & 3
    odd = (turn & 1) == 1
    cos_part = jnp.where(odd, sin_poly, cos_poly)
    sin_part = jnp.where(odd, cos_poly, sin_poly)
    return jnp.where((turn == 1) | (turn == 2), -cos_part, cos_part), jnp.where(turn >= 2, -sin_part, sin_part)


def rotary_tables(positions, head_dim):
    half_dim = head_dim // 2
    inv_freq = 10000.0 ** (-2.0 * jnp.arange(half_dim, dtype=jnp.float32) / head_dim)
    sign = jnp.where(jnp.arange(head_dim) < half_dim, -1.0, 1.0).astype(jnp.float32)
    angles = positions.reshape(-1, 1).astype(jnp.float32) * jnp.concatenate([inv_freq, inv_freq])
    cos_tab, sin_tab = cos_sin(angles)
    return cos_tab, sin_tab * sign


def group_signal(me, n_cp):
    barrier = pltpu.get_barrier_semaphore()

    def signal(k, _):
        pl.semaphore_signal(barrier, inc=1, device_id={AXIS: lax.rem(me + k, n_cp)}, device_id_type=pl.DeviceIdType.MESH)
        return 0

    lax.fori_loop(1, n_cp, signal, 0)


def put(src, dst, owner, me, send_sem, recv_sem):
    @pl.when(owner == me)
    def _():
        pltpu.make_async_copy(src, dst, recv_sem).start()

    @pl.when(owner != me)
    def _():
        pltpu.make_async_remote_copy(src, dst, send_sem, recv_sem, device_id={AXIS: owner}, device_id_type=pl.DeviceIdType.MESH).start()


def wait_bytes_of(ref, sem):
    pltpu.make_async_copy(ref, ref, sem).wait()


def block_kernel(
    n_cp, x_ref, gain_ref, cos_ref, sin_ref, wq_ref, wk_ref, wv_ref, wo_ref, y_ref,
    h_ref, w_buf, acc, stage, q_in, kv_in, v_t, o_stage, s_buf, p_buf, o_acc, stat, o_in, y_buf,
    w_sem, y_sem, send_q, send_kv, send_o, send_half, recv_q, recv_kv, recv_o, recv_half,
):
    me = lax.axis_index(AXIS)
    chip, core = me // 2, lax.rem(me, 2)
    n_steps, batch, seq, width = stage.shape
    rounds, total, _ = q_in.shape
    per_round = batch // rounds
    n_q = n_cp // per_round
    n_kv = n_steps - n_q
    head_dim = width // 2
    half_dim = head_dim // 2
    blk_q = s_buf.shape[1] // 2
    blk_k = s_buf.shape[0]
    n_blocks = total // blk_q
    ratio = blk_k // blk_q
    span = blk_q // seq
    chips_per_k = blk_k // (2 * seq)
    factor = LOG2E * head_dim ** -0.5

    def kv_block(step):
        return lax.rem(step + chip, n_kv)

    def q_block(step):
        return lax.rem(step - n_kv + chip, n_q)

    def fetch(step, slot):
        @pl.when(step < n_kv)
        def _():
            cols = pl.ds(pl.multiple_of(kv_block(step) * head_dim, head_dim), head_dim)
            pltpu.make_async_copy(wk_ref.at[:, cols], w_buf.at[slot, :, pl.ds(0, head_dim)], w_sem.at[slot]).start()
            pltpu.make_async_copy(wv_ref.at[:, cols], w_buf.at[slot, :, pl.ds(head_dim, head_dim)], w_sem.at[slot]).start()

        @pl.when(step >= n_kv)
        def _():
            cols = pl.ds(pl.multiple_of(q_block(step) * width, width), width)
            pltpu.make_async_copy(wq_ref.at[:, cols], w_buf.at[slot], w_sem.at[slot]).start()

    def send_kv_tiles(step):
        for b in range(batch):
            owner = 2 * (b % per_round * n_kv + kv_block(step)) + core
            r = b // per_round
            put(stage.at[step, b], kv_in.at[r, chip, core], owner, me, send_kv, recv_kv.at[r])

    def send_q_tiles(step, r):
        for k in range(per_round):
            put(stage.at[step, r * per_round + k], q_in.at[r, pl.ds(me * seq, seq)], k * n_q + q_block(step), me, send_q, recv_q.at[r])

    def send_first(step):
        @pl.when(step < n_kv)
        def _():
            send_kv_tiles(step)

        @pl.when(step >= n_kv)
        def _():
            send_q_tiles(step, 0)

    fetch(0, 0)
    group_signal(me, n_cp)

    def norm(k, _):
        rows = pl.ds(pl.multiple_of(k * NORM_ROWS, NORM_ROWS), NORM_ROWS)
        x = x_ref[rows, :].astype(jnp.float32)
        inv_rms = lax.rsqrt(jnp.mean(x * x, axis=-1, keepdims=True) + 1e-5)
        h_ref[rows, :] = (x * inv_rms * gain_ref[...].astype(jnp.float32)).astype(jnp.bfloat16)
        return 0

    lax.fori_loop(0, batch * seq // NORM_ROWS, norm, 0)
    pl.semaphore_wait(pltpu.get_barrier_semaphore(), n_cp - 1)

    def rotate(x):
        return (x * cos_ref[...] + pltpu.roll(x, half_dim, 1) * sin_ref[...]).astype(jnp.bfloat16).reshape(batch, seq, head_dim)

    def project(step, _):
        slot = lax.rem(step, 2)
        wait_bytes_of(w_buf.at[slot], w_sem.at[slot])

        @pl.when(step + 1 < n_steps)
        def _():
            fetch(step + 1, 1 - slot)

        acc[...] = jnp.dot(h_ref[...], w_buf[slot], preferred_element_type=jnp.float32)
        stage[step, :, :, 0:head_dim] = rotate(acc[:, 0:head_dim])

        @pl.when(step < n_kv)
        def _():
            stage[step, :, :, head_dim:width] = acc[:, head_dim:width].astype(jnp.bfloat16).reshape(batch, seq, head_dim)

        @pl.when(step >= n_kv)
        def _():
            stage[step, :, :, head_dim:width] = rotate(acc[:, head_dim:width])

        @pl.when(step > 0)
        def _():
            send_first(step - 1)

        return 0

    lax.fori_loop(0, n_steps, project, 0)
    send_first(n_steps - 1)

    def swap(r, _):
        wait_bytes_of(kv_in.at[r, :, 0], recv_kv.at[r])
        mine = kv_in.at[r, :, core]
        pltpu.make_async_remote_copy(mine, mine, send_half, recv_half.at[r], device_id={AXIS: me + 1 - 2 * core}, device_id_type=pl.DeviceIdType.MESH).start()
        return 0

    lax.fori_loop(0, rounds, swap, 0)

    def send_rest(k, _):
        send_q_tiles(n_kv + lax.rem(k, n_q), 1 + k // n_q)
        return 0

    lax.fori_loop(0, (rounds - 1) * n_q, send_rest, 0)

    def out_fetch(k, slot):
        cols = pl.ds(pl.multiple_of(lax.rem(k, n_out) * width, width), width)
        pltpu.make_async_copy(wo_ref.at[:, cols], w_buf.at[slot], w_sem.at[slot]).start()

    n_out = wo_ref.shape[1] // width
    out_fetch(0, 0)

    def place(t):
        i = lax.rem(t + chip + 1, n_blocks)
        return i, i // ratio

    def attend(r, _):
        wait_bytes_of(q_in.at[r], recv_q.at[r])
        wait_bytes_of(kv_in.at[r, :, 0], recv_half.at[r])

        def kv_rows(j, lanes):
            return kv_in[r, pl.ds(j * chips_per_k, chips_per_k), :, :, lanes].reshape(blk_k, head_dim)

        def turn(j, _):
            v_t[:, pl.ds(pl.multiple_of(j * blk_k, blk_k), blk_k)] = kv_rows(j, slice(head_dim, width)).astype(jnp.float32).T.astype(jnp.bfloat16)
            return 0

        lax.fori_loop(0, total // blk_k, turn, 0)

        def send(t):
            i, _ = place(t)
            b = r * per_round + me // n_q
            cols = pl.ds(pl.multiple_of(lax.rem(me, n_q) * width, width), width)
            for s in range(span):
                owner = i * span + s
                put(o_stage.at[r, pl.ds(owner * seq, seq)], o_in.at[b, :, cols], owner, me, send_o, recv_o.at[r])

        def next_scores(i, j):
            k_blk = kv_rows(j, slice(0, head_dim))
            q_rows = pl.ds(pl.multiple_of(i * blk_q, blk_q), blk_q)
            for g in range(2):
                q_head = q_in[r, q_rows, g * head_dim:(g + 1) * head_dim]
                cols = slice(g * blk_q, (g + 1) * blk_q)
                s = lax.dot_general(k_blk, q_head, (((1,), (1,)), ((), ())), preferred_element_type=jnp.float32)
                s_buf[:, cols] = s
                stat[3, 0:1, cols] = jnp.max(s, axis=0, keepdims=True)

        def weighed(j):
            cols = pl.ds(pl.multiple_of(j * blk_k, blk_k), blk_k)
            return o_acc[...] * stat[2, 0:1, :] + jnp.dot(v_t[:, cols], p_buf[...], preferred_element_type=jnp.float32)

        def finish(t):
            i, n_full = place(t)
            out = weighed(jnp.maximum(n_full - 1, 0)) * (1.0 / stat[1, 0:1, :])
            q_rows = pl.ds(pl.multiple_of(i * blk_q, blk_q), blk_q)
            for g in range(2):
                o_stage[r, q_rows, g * head_dim:(g + 1) * head_dim] = out[:, g * blk_q:(g + 1) * blk_q].T.astype(jnp.bfloat16)

        def step(t, _):
            i, n_full = place(t)
            after = place(jnp.minimum(t + 1, n_blocks - 1))

            def follow(n_done):
                more = n_done < n_full
                next_scores(jnp.where(more, i, after[0]), jnp.where(more, n_done, after[1]))

            @pl.when(t > 1)
            def _():
                send(t - 2)

            def diagonal(size):
                finish(jnp.maximum(t - 1, 0))
                o_acc[...] = jnp.zeros_like(o_acc)
                shape = (size, 2 * blk_q)
                allowed = lax.broadcasted_iota(jnp.int32, shape, 0) - (size - blk_q) <= lax.rem(lax.broadcasted_iota(jnp.int32, shape, 1), blk_q)
                s = jnp.where(allowed, s_buf[0:size, :], -jnp.inf)
                top = jnp.max(s, axis=0, keepdims=True)
                prob = jnp.exp2(s * factor - top * factor)
                stat[0, 0:1, :] = top
                stat[1, 0:1, :] = jnp.sum(prob, axis=0, keepdims=True)
                stat[2, 0:1, :] = jnp.ones_like(top)
                p_buf[0:size, :] = prob.astype(jnp.bfloat16)
                if size < blk_k:
                    p_buf[size:blk_k, :] = jnp.zeros((blk_k - size, 2 * blk_q), jnp.bfloat16)
                follow(0)

            for part in range(ratio):
                pl.when(lax.rem(i, ratio) == part)(functools.partial(diagonal, (part + 1) * blk_q))

            def full(j, _):
                o_acc[...] = weighed(jnp.where(j == 0, n_full, j - 1))
                top = stat[0, 0:1, :]
                new_top = jnp.maximum(top, stat[3, 0:1, :])
                shift = new_top * factor
                rescale = jnp.exp2(top * factor - shift)
                part_sum = jnp.zeros((8, 2 * blk_q), jnp.float32)
                for k in range(0, blk_k, CHUNK):
                    prob = jnp.exp2(s_buf[k:k + CHUNK, :] * factor - shift)
                    part_sum = part_sum + jnp.sum(prob.reshape(CHUNK // 8, 8, 2 * blk_q), axis=0)
                    p_buf[k:k + CHUNK, :] = prob.astype(jnp.bfloat16)
                stat[0, 0:1, :] = new_top
                stat[1, 0:1, :] = stat[1, 0:1, :] * rescale + jnp.sum(part_sum, axis=0, keepdims=True)
                stat[2, 0:1, :] = rescale
                follow(j + 1)
                return 0

            lax.fori_loop(0, n_full, full, 0)
            return 0

        o_acc[...] = jnp.zeros_like(o_acc)
        stat[...] = jnp.ones_like(stat)
        p_buf[...] = jnp.zeros_like(p_buf)
        next_scores(*place(0))
        lax.fori_loop(0, n_blocks, step, 0)
        send(n_blocks - 2)
        finish(n_blocks - 1)
        send(n_blocks - 1)
        return 0

    lax.fori_loop(0, rounds, attend, 0)

    def y_copy(k, slot):
        r, cols = k // n_out, pl.ds(pl.multiple_of(lax.rem(k, n_out) * width, width), width)
        return pltpu.make_async_copy(y_buf.at[slot], y_ref.at[pl.ds(r * per_round, per_round), :, cols], y_sem.at[slot])

    def out_project(k, _):
        slot, r = lax.rem(k, 2), k // n_out

        @pl.when(k + 1 < rounds * n_out)
        def _():
            out_fetch(k + 1, 1 - slot)

        @pl.when(lax.rem(k, n_out) == 0)
        def _():
            wait_bytes_of(o_in.at[pl.ds(r * per_round, per_round)], recv_o.at[r])

        wait_bytes_of(w_buf.at[slot], w_sem.at[slot])

        @pl.when(k > 1)
        def _():
            y_copy(k - 2, slot).wait()

        attn = o_in[pl.ds(r * per_round, per_round)].reshape(per_round * seq, wo_ref.shape[0])
        proj = jnp.dot(attn, w_buf[slot], preferred_element_type=jnp.float32)
        rows = pl.ds(pl.multiple_of(r * per_round * seq, seq), per_round * seq)
        cols = pl.ds(pl.multiple_of(lax.rem(k, n_out) * width, width), width)
        y_buf[slot] = (x_ref[rows, cols].astype(jnp.float32) + proj).astype(jnp.bfloat16).reshape(per_round, seq, width)
        y_copy(k, slot).start()
        return 0

    lax.fori_loop(0, rounds * n_out, out_project, 0)
    for k in (rounds * n_out - 2, rounds * n_out - 1):
        y_copy(k, k % 2).wait()
    away = (n_cp - 1) * seq
    wait_bytes_of(q_in.at[:, pl.ds(0, away)], send_q)
    wait_bytes_of(kv_in.at[:, pl.ds(0, n_cp // 2 - 1), 0], send_kv)
    wait_bytes_of(o_stage.at[:, pl.ds(0, away)], send_o)
    wait_bytes_of(kv_in.at[:, :, 0], send_half)


def solution(mesh):
    n_cp = mesh.shape[AXIS]

    def local_block(hidden, positions, norm_gain, w_query, w_key, w_value, w_out):
        batch, seq, model_dim = hidden.shape
        n_heads, head_dim, _ = w_out.shape
        n_kv = w_key.shape[1] // head_dim
        width = 2 * head_dim
        n_q = n_heads // 2
        rounds = batch * n_q // n_cp
        per_round = batch // rounds
        total = n_cp * seq
        n_steps = n_kv + n_q
        blk_q = 2 * seq
        blk_k = 2 * blk_q
        any_space = pl.BlockSpec(memory_space=pl.ANY)
        vmem = pl.BlockSpec(memory_space=pltpu.VMEM)
        cos_tab, sin_tab = rotary_tables(positions, head_dim)
        dma = pltpu.SemaphoreType.DMA
        return pl.pallas_call(
            functools.partial(block_kernel, n_cp),
            out_shape=jax.ShapeDtypeStruct(hidden.shape, jnp.bfloat16),
            in_specs=[vmem] * 4 + [any_space] * 4,
            out_specs=any_space,
            scratch_shapes=[
                pltpu.VMEM((batch * seq, model_dim), jnp.bfloat16),
                pltpu.VMEM((2, model_dim, width), jnp.bfloat16),
                pltpu.VMEM((batch * seq, width), jnp.float32),
                pltpu.VMEM((n_steps, batch, seq, width), jnp.bfloat16),
                pltpu.VMEM((rounds, total, width), jnp.bfloat16),
                pltpu.VMEM((rounds, n_cp // 2, 2, seq, width), jnp.bfloat16),
                pltpu.VMEM((head_dim, total), jnp.bfloat16),
                pltpu.VMEM((rounds, total, width), jnp.bfloat16),
                pltpu.VMEM((blk_k, 2 * blk_q), jnp.float32),
                pltpu.VMEM((blk_k, 2 * blk_q), jnp.bfloat16),
                pltpu.VMEM((head_dim, 2 * blk_q), jnp.float32),
                pltpu.VMEM((4, 8, 2 * blk_q), jnp.float32),
                pltpu.VMEM((batch, seq, n_heads * head_dim), jnp.bfloat16),
                pltpu.VMEM((2, per_round, seq, width), jnp.bfloat16),
                dma((2,)), dma((2,)),
                dma, dma, dma, dma,
                dma((rounds,)), dma((rounds,)), dma((rounds,)), dma((rounds,)),
            ],
            compiler_params=pltpu.CompilerParams(collective_id=0, has_side_effects=True, vmem_limit_bytes=VMEM_LIMIT),
            name='attention_block',
        )(hidden.reshape(batch * seq, model_dim), norm_gain.reshape(1, model_dim), cos_tab, sin_tab, w_query, w_key, w_value, w_out.reshape(n_heads * head_dim, model_dim))

    act_spec = P('dp', 'cp', None)
    return jax.shard_map(local_block, mesh=mesh, in_specs=(act_spec, P('dp', 'cp'), P(), P(), P(), P(), P()), out_specs=act_spec, check_vma=False)
```

```python
import functools

import jax
import jax.numpy as jnp
from jax import lax
from jax.experimental import pallas as pl
from jax.experimental.pallas import tpu as pltpu
from jax.sharding import PartitionSpec as P

AXIS = 'cp'
LOG2E = 1.4426950408889634
CHUNK = 32
NORM_ROWS = 32
VMEM_LIMIT = 60 * 1024 * 1024


def cos_sin(angles):
    quarter = jnp.round(angles * 0.6366197723675814)
    rest = ((angles - quarter * 1.5703125) - quarter * 4.837512969970703e-4) - quarter * 7.549789954891626e-8
    square = rest * rest
    sin_poly = rest + rest * square * (-1.6666654611e-1 + square * (8.3321608736e-3 - square * 1.9515295891e-4))
    cos_poly = 1.0 - 0.5 * square + square * square * (4.166664568298827e-2 + square * (-1.388731625493765e-3 + square * 2.443315711809948e-5))
    turn = quarter.astype(jnp.int32) & 3
    odd = (turn & 1) == 1
    cos_part = jnp.where(odd, sin_poly, cos_poly)
    sin_part = jnp.where(odd, cos_poly, sin_poly)
    return jnp.where((turn == 1) | (turn == 2), -cos_part, cos_part), jnp.where(turn >= 2, -sin_part, sin_part)


def rotary_tables(positions, head_dim):
    half_dim = head_dim // 2
    inv_freq = 10000.0 ** (-2.0 * jnp.arange(half_dim, dtype=jnp.float32) / head_dim)
    sign = jnp.where(jnp.arange(head_dim) < half_dim, -1.0, 1.0).astype(jnp.float32)
    angles = positions.reshape(-1, 1).astype(jnp.float32) * jnp.concatenate([inv_freq, inv_freq])
    cos_tab, sin_tab = cos_sin(angles)
    return cos_tab, sin_tab * sign


def group_signal(me, n_cp):
    barrier = pltpu.get_barrier_semaphore()

    def signal(k, _):
        pl.semaphore_signal(barrier, inc=1, device_id={AXIS: lax.rem(me + k, n_cp)}, device_id_type=pl.DeviceIdType.MESH)
        return 0

    lax.fori_loop(1, n_cp, signal, 0)


def put(src, dst, owner, me, send_sem, recv_sem):
    @pl.when(owner == me)
    def _():
        pltpu.make_async_copy(src, dst, recv_sem).start()

    @pl.when(owner != me)
    def _():
        pltpu.make_async_remote_copy(src, dst, send_sem, recv_sem, device_id={AXIS: owner}, device_id_type=pl.DeviceIdType.MESH).start()


def wait_bytes_of(ref, sem):
    pltpu.make_async_copy(ref, ref, sem).wait()


def block_kernel(
    n_cp, x_ref, gain_ref, cos_ref, sin_ref, wq_ref, wk_ref, wv_ref, wo_ref, y_ref,
    h_ref, w_buf, acc, stage, q_in, kv_in, v_t, o_stage, s_buf, p_buf, o_acc, stat, o_in, y_buf,
    w_sem, y_sem, send_q, send_kv, send_o, send_half, recv_q, recv_kv, recv_o, recv_half,
):
    me = lax.axis_index(AXIS)
    chip, core = me // 2, lax.rem(me, 2)
    n_steps, batch, seq, width = stage.shape
    rounds, total, _ = q_in.shape
    per_round = batch // rounds
    n_q = n_cp // per_round
    n_kv = n_steps - n_q
    head_dim = width // 2
    half_dim = head_dim // 2
    blk_q = s_buf.shape[1] // 2
    blk_k = s_buf.shape[0]
    n_blocks = total // blk_q
    ratio = blk_k // blk_q
    span = blk_q // seq
    chips_per_k = blk_k // (2 * seq)
    factor = LOG2E * head_dim ** -0.5

    def kv_block(step):
        return lax.rem(step + chip, n_kv)

    def q_block(step):
        return lax.rem(step - n_kv + chip, n_q)

    def fetch(step, slot):
        @pl.when(step < n_kv)
        def _():
            cols = pl.ds(pl.multiple_of(kv_block(step) * head_dim, head_dim), head_dim)
            pltpu.make_async_copy(wk_ref.at[:, cols], w_buf.at[slot, :, pl.ds(0, head_dim)], w_sem.at[slot]).start()
            pltpu.make_async_copy(wv_ref.at[:, cols], w_buf.at[slot, :, pl.ds(head_dim, head_dim)], w_sem.at[slot]).start()

        @pl.when(step >= n_kv)
        def _():
            cols = pl.ds(pl.multiple_of(q_block(step) * width, width), width)
            pltpu.make_async_copy(wq_ref.at[:, cols], w_buf.at[slot], w_sem.at[slot]).start()

    def send_kv_tiles(step, first, last):
        for b in range(first * per_round, last * per_round):
            owner = 2 * (b % per_round * n_kv + kv_block(step)) + core
            r = b // per_round
            put(stage.at[step, b], kv_in.at[r, chip, core], owner, me, send_kv, recv_kv.at[r])

    def send_q_tiles(step, r):
        for k in range(per_round):
            put(stage.at[step, r * per_round + k], q_in.at[r, pl.ds(me * seq, seq)], k * n_q + q_block(step), me, send_q, recv_q.at[r])

    early = min(2, rounds)

    def send_first(step):
        @pl.when(step < n_kv)
        def _():
            send_kv_tiles(step, 0, early)

        @pl.when(step >= n_kv)
        def _():
            send_q_tiles(step, 0)

    fetch(0, 0)
    group_signal(me, n_cp)

    def norm(k, _):
        rows = pl.ds(pl.multiple_of(k * NORM_ROWS, NORM_ROWS), NORM_ROWS)
        x = x_ref[rows, :].astype(jnp.float32)
        inv_rms = lax.rsqrt(jnp.mean(x * x, axis=-1, keepdims=True) + 1e-5)
        h_ref[rows, :] = (x * inv_rms * gain_ref[...].astype(jnp.float32)).astype(jnp.bfloat16)
        return 0

    lax.fori_loop(0, batch * seq // NORM_ROWS, norm, 0)
    pl.semaphore_wait(pltpu.get_barrier_semaphore(), n_cp - 1)

    def rotate(x):
        return (x * cos_ref[...] + pltpu.roll(x, half_dim, 1) * sin_ref[...]).astype(jnp.bfloat16).reshape(batch, seq, head_dim)

    def project(step, _):
        slot = lax.rem(step, 2)
        wait_bytes_of(w_buf.at[slot], w_sem.at[slot])

        @pl.when(step + 1 < n_steps)
        def _():
            fetch(step + 1, 1 - slot)

        acc[...] = jnp.dot(h_ref[...], w_buf[slot], preferred_element_type=jnp.float32)
        stage[step, :, :, 0:head_dim] = rotate(acc[:, 0:head_dim])

        @pl.when(step < n_kv)
        def _():
            stage[step, :, :, head_dim:width] = acc[:, head_dim:width].astype(jnp.bfloat16).reshape(batch, seq, head_dim)

        @pl.when(step >= n_kv)
        def _():
            stage[step, :, :, head_dim:width] = rotate(acc[:, head_dim:width])

        @pl.when(step > 0)
        def _():
            send_first(step - 1)

        return 0

    lax.fori_loop(0, n_steps, project, 0)
    send_first(n_steps - 1)

    def swap(r, _):
        wait_bytes_of(kv_in.at[r, :, 0], recv_kv.at[r])
        mine = kv_in.at[r, :, core]
        pltpu.make_async_remote_copy(mine, mine, send_half, recv_half.at[r], device_id={AXIS: me + 1 - 2 * core}, device_id_type=pl.DeviceIdType.MESH).start()
        return 0

    lax.fori_loop(0, early, swap, 0)

    def send_rest(k, _):
        send_q_tiles(n_kv + lax.rem(k, n_q), 1 + k // n_q)

        @pl.when(k < n_kv)
        def _():
            send_kv_tiles(k, early, rounds)

        return 0

    lax.fori_loop(0, (rounds - 1) * n_q, send_rest, 0)

    def out_fetch(k, slot):
        cols = pl.ds(pl.multiple_of(lax.rem(k, n_out) * width, width), width)
        pltpu.make_async_copy(wo_ref.at[:, cols], w_buf.at[slot], w_sem.at[slot]).start()

    n_out = wo_ref.shape[1] // width
    out_fetch(0, 0)

    def place(t):
        i = lax.rem(t + me // span + 1, n_blocks)
        return i, i // ratio

    def attend(r, _):
        @pl.when((r + 1 >= early) & (r + 1 < rounds))
        def _():
            swap(r + 1, 0)

        wait_bytes_of(q_in.at[r], recv_q.at[r])
        wait_bytes_of(kv_in.at[r, :, 0], recv_half.at[r])

        def kv_rows(j, lanes):
            return kv_in[r, pl.ds(j * chips_per_k, chips_per_k), :, :, lanes].reshape(blk_k, head_dim)

        def turn(j, _):
            v_t[:, pl.ds(pl.multiple_of(j * blk_k, blk_k), blk_k)] = kv_rows(j, slice(head_dim, width)).astype(jnp.float32).T.astype(jnp.bfloat16)
            return 0

        lax.fori_loop(0, total // blk_k, turn, 0)

        def send(t):
            i, _ = place(t)
            b = r * per_round + me // n_q
            cols = pl.ds(pl.multiple_of(lax.rem(me, n_q) * width, width), width)
            for s in range(span):
                owner = i * span + s
                put(o_stage.at[r, pl.ds(owner * seq, seq)], o_in.at[b, :, cols], owner, me, send_o, recv_o.at[r])

        def next_scores(i, j):
            k_blk = kv_rows(j, slice(0, head_dim))
            q_rows = pl.ds(pl.multiple_of(i * blk_q, blk_q), blk_q)
            for g in range(2):
                q_head = q_in[r, q_rows, g * head_dim:(g + 1) * head_dim]
                cols = slice(g * blk_q, (g + 1) * blk_q)
                s = lax.dot_general(k_blk, q_head, (((1,), (1,)), ((), ())), preferred_element_type=jnp.float32)
                s_buf[:, cols] = s
                stat[3, 0:1, cols] = jnp.max(s, axis=0, keepdims=True)

        def weighed(j):
            cols = pl.ds(pl.multiple_of(j * blk_k, blk_k), blk_k)
            return o_acc[...] * stat[2, 0:1, :] + jnp.dot(v_t[:, cols], p_buf[...], preferred_element_type=jnp.float32)

        def finish(t):
            i, n_full = place(t)
            out = weighed(jnp.maximum(n_full - 1, 0)) * (1.0 / stat[1, 0:1, :])
            q_rows = pl.ds(pl.multiple_of(i * blk_q, blk_q), blk_q)
            for g in range(2):
                o_stage[r, q_rows, g * head_dim:(g + 1) * head_dim] = out[:, g * blk_q:(g + 1) * blk_q].T.astype(jnp.bfloat16)

        def step(t, _):
            i, n_full = place(t)
            after = place(jnp.minimum(t + 1, n_blocks - 1))

            def follow(n_done):
                more = n_done < n_full
                next_scores(jnp.where(more, i, after[0]), jnp.where(more, n_done, after[1]))

            @pl.when(t > 1)
            def _():
                send(t - 2)

            def diagonal(size):
                finish(jnp.maximum(t - 1, 0))
                o_acc[...] = jnp.zeros_like(o_acc)
                shape = (size, 2 * blk_q)
                allowed = lax.broadcasted_iota(jnp.int32, shape, 0) - (size - blk_q) <= lax.rem(lax.broadcasted_iota(jnp.int32, shape, 1), blk_q)
                s = jnp.where(allowed, s_buf[0:size, :], -jnp.inf)
                top = jnp.max(s, axis=0, keepdims=True)
                prob = jnp.exp2(s * factor - top * factor)
                stat[0, 0:1, :] = top
                stat[1, 0:1, :] = jnp.sum(prob, axis=0, keepdims=True)
                stat[2, 0:1, :] = jnp.ones_like(top)
                p_buf[0:size, :] = prob.astype(jnp.bfloat16)
                if size < blk_k:
                    p_buf[size:blk_k, :] = jnp.zeros((blk_k - size, 2 * blk_q), jnp.bfloat16)
                follow(0)

            for part in range(ratio):
                pl.when(lax.rem(i, ratio) == part)(functools.partial(diagonal, (part + 1) * blk_q))

            def full(j, _):
                o_acc[...] = weighed(jnp.where(j == 0, n_full, j - 1))
                top = stat[0, 0:1, :]
                new_top = jnp.maximum(top, stat[3, 0:1, :])
                shift = new_top * factor
                rescale = jnp.exp2(top * factor - shift)
                part_sum = jnp.zeros((8, 2 * blk_q), jnp.float32)
                for k in range(0, blk_k, CHUNK):
                    prob = jnp.exp2(s_buf[k:k + CHUNK, :] * factor - shift)
                    part_sum = part_sum + jnp.sum(prob.reshape(CHUNK // 8, 8, 2 * blk_q), axis=0)
                    p_buf[k:k + CHUNK, :] = prob.astype(jnp.bfloat16)
                stat[0, 0:1, :] = new_top
                stat[1, 0:1, :] = stat[1, 0:1, :] * rescale + jnp.sum(part_sum, axis=0, keepdims=True)
                stat[2, 0:1, :] = rescale
                follow(j + 1)
                return 0

            lax.fori_loop(0, n_full, full, 0)
            return 0

        o_acc[...] = jnp.zeros_like(o_acc)
        stat[...] = jnp.ones_like(stat)
        p_buf[...] = jnp.zeros_like(p_buf)
        next_scores(*place(0))
        lax.fori_loop(0, n_blocks, step, 0)
        send(n_blocks - 2)
        finish(n_blocks - 1)
        send(n_blocks - 1)
        return 0

    lax.fori_loop(0, rounds, attend, 0)

    def y_copy(k, slot):
        r, cols = k // n_out, pl.ds(pl.multiple_of(lax.rem(k, n_out) * width, width), width)
        return pltpu.make_async_copy(y_buf.at[slot], y_ref.at[pl.ds(r * per_round, per_round), :, cols], y_sem.at[slot])

    def out_project(k, _):
        slot, r = lax.rem(k, 2), k // n_out

        @pl.when(k + 1 < rounds * n_out)
        def _():
            out_fetch(k + 1, 1 - slot)

        @pl.when(lax.rem(k, n_out) == 0)
        def _():
            wait_bytes_of(o_in.at[pl.ds(r * per_round, per_round)], recv_o.at[r])

        wait_bytes_of(w_buf.at[slot], w_sem.at[slot])

        @pl.when(k > 1)
        def _():
            y_copy(k - 2, slot).wait()

        attn = o_in[pl.ds(r * per_round, per_round)].reshape(per_round * seq, wo_ref.shape[0])
        proj = jnp.dot(attn, w_buf[slot], preferred_element_type=jnp.float32)
        rows = pl.ds(pl.multiple_of(r * per_round * seq, seq), per_round * seq)
        cols = pl.ds(pl.multiple_of(lax.rem(k, n_out) * width, width), width)
        y_buf[slot] = (x_ref[rows, cols].astype(jnp.float32) + proj).astype(jnp.bfloat16).reshape(per_round, seq, width)
        y_copy(k, slot).start()
        return 0

    lax.fori_loop(0, rounds * n_out, out_project, 0)
    for k in (rounds * n_out - 2, rounds * n_out - 1):
        y_copy(k, k % 2).wait()
    away = (n_cp - 1) * seq
    wait_bytes_of(q_in.at[:, pl.ds(0, away)], send_q)
    wait_bytes_of(kv_in.at[:, pl.ds(0, n_cp // 2 - 1), 0], send_kv)
    wait_bytes_of(o_stage.at[:, pl.ds(0, away)], send_o)
    wait_bytes_of(kv_in.at[:, :, 0], send_half)


def solution(mesh):
    n_cp = mesh.shape[AXIS]

    def local_block(hidden, positions, norm_gain, w_query, w_key, w_value, w_out):
        batch, seq, model_dim = hidden.shape
        n_heads, head_dim, _ = w_out.shape
        n_kv = w_key.shape[1] // head_dim
        width = 2 * head_dim
        n_q = n_heads // 2
        rounds = batch * n_q // n_cp
        per_round = batch // rounds
        total = n_cp * seq
        n_steps = n_kv + n_q
        blk_q = 4 * seq
        blk_k = blk_q
        any_space = pl.BlockSpec(memory_space=pl.ANY)
        vmem = pl.BlockSpec(memory_space=pltpu.VMEM)
        cos_tab, sin_tab = rotary_tables(positions, head_dim)
        dma = pltpu.SemaphoreType.DMA
        return pl.pallas_call(
            functools.partial(block_kernel, n_cp),
            out_shape=jax.ShapeDtypeStruct(hidden.shape, jnp.bfloat16),
            in_specs=[vmem] * 4 + [any_space] * 4,
            out_specs=any_space,
            scratch_shapes=[
                pltpu.VMEM((batch * seq, model_dim), jnp.bfloat16),
                pltpu.VMEM((2, model_dim, width), jnp.bfloat16),
                pltpu.VMEM((batch * seq, width), jnp.float32),
                pltpu.VMEM((n_steps, batch, seq, width), jnp.bfloat16),
                pltpu.VMEM((rounds, total, width), jnp.bfloat16),
                pltpu.VMEM((rounds, n_cp // 2, 2, seq, width), jnp.bfloat16),
                pltpu.VMEM((head_dim, total), jnp.bfloat16),
                pltpu.VMEM((rounds, total, width), jnp.bfloat16),
                pltpu.VMEM((blk_k, 2 * blk_q), jnp.float32),
                pltpu.VMEM((blk_k, 2 * blk_q), jnp.bfloat16),
                pltpu.VMEM((head_dim, 2 * blk_q), jnp.float32),
                pltpu.VMEM((4, 8, 2 * blk_q), jnp.float32),
                pltpu.VMEM((batch, seq, n_heads * head_dim), jnp.bfloat16),
                pltpu.VMEM((2, per_round, seq, width), jnp.bfloat16),
                dma((2,)), dma((2,)),
                dma, dma, dma, dma,
                dma((rounds,)), dma((rounds,)), dma((rounds,)), dma((rounds,)),
            ],
            compiler_params=pltpu.CompilerParams(collective_id=0, has_side_effects=True, vmem_limit_bytes=VMEM_LIMIT),
            name='attention_block',
        )(hidden.reshape(batch * seq, model_dim), norm_gain.reshape(1, model_dim), cos_tab, sin_tab, w_query, w_key, w_value, w_out.reshape(n_heads * head_dim, model_dim))

    act_spec = P('dp', 'cp', None)
    return jax.shard_map(local_block, mesh=mesh, in_specs=(act_spec, P('dp', 'cp'), P(), P(), P(), P(), P()), out_specs=act_spec, check_vma=False)
```

```python
import functools

import jax
import jax.numpy as jnp
from jax import lax
from jax.experimental import pallas as pl
from jax.experimental.pallas import tpu as pltpu
from jax.sharding import PartitionSpec as P

AXIS = 'cp'
LOG2E = 1.4426950408889634
CHUNK = 32
NORM_ROWS = 32
VMEM_LIMIT = 60 * 1024 * 1024


def cos_sin(angles):
    quarter = jnp.round(angles * 0.6366197723675814)
    rest = ((angles - quarter * 1.5703125) - quarter * 4.837512969970703e-4) - quarter * 7.549789954891626e-8
    square = rest * rest
    sin_poly = rest + rest * square * (-1.6666654611e-1 + square * (8.3321608736e-3 - square * 1.9515295891e-4))
    cos_poly = 1.0 - 0.5 * square + square * square * (4.166664568298827e-2 + square * (-1.388731625493765e-3 + square * 2.443315711809948e-5))
    turn = quarter.astype(jnp.int32) & 3
    odd = (turn & 1) == 1
    cos_part = jnp.where(odd, sin_poly, cos_poly)
    sin_part = jnp.where(odd, cos_poly, sin_poly)
    return jnp.where((turn == 1) | (turn == 2), -cos_part, cos_part), jnp.where(turn >= 2, -sin_part, sin_part)


def rotary_tables(positions, head_dim):
    half_dim = head_dim // 2
    inv_freq = 10000.0 ** (-2.0 * jnp.arange(half_dim, dtype=jnp.float32) / head_dim)
    sign = jnp.where(jnp.arange(head_dim) < half_dim, -1.0, 1.0).astype(jnp.float32)
    angles = positions.astype(jnp.float32)[:, :, None] * jnp.concatenate([inv_freq, inv_freq])
    cos_tab, sin_tab = cos_sin(angles)
    return cos_tab.reshape(-1, head_dim), (sin_tab * sign).reshape(-1, head_dim)


def group_signal(me, n_cp):
    barrier = pltpu.get_barrier_semaphore()

    def signal(k, _):
        pl.semaphore_signal(barrier, inc=1, device_id={AXIS: lax.rem(me + k, n_cp)}, device_id_type=pl.DeviceIdType.MESH)
        return 0

    lax.fori_loop(1, n_cp, signal, 0)


def put(src, dst, owner, me, send_sem, recv_sem):
    @pl.when(owner == me)
    def _():
        pltpu.make_async_copy(src, dst, recv_sem).start()

    @pl.when(owner != me)
    def _():
        pltpu.make_async_remote_copy(src, dst, send_sem, recv_sem, device_id={AXIS: owner}, device_id_type=pl.DeviceIdType.MESH).start()


def wait_bytes_of(ref, sem):
    pltpu.make_async_copy(ref, ref, sem).wait()


def block_kernel(
    n_cp, x_ref, gain_ref, cos_ref, sin_ref, wq_ref, wk_ref, wv_ref, wo_ref, y_ref,
    h_ref, w_buf, acc, stage, q_in, kv_in, v_t, o_stage, s_buf, p_buf, o_acc, stat, o_in, y_buf,
    w_sem, y_sem, send_q, send_kv, send_o, send_half, recv_q, recv_kv, recv_o, recv_half,
):
    me = lax.axis_index(AXIS)
    chip, core = me // 2, lax.rem(me, 2)
    n_steps, batch, seq, width = stage.shape
    rounds, total, _ = q_in.shape
    per_round = batch // rounds
    n_q = n_cp // per_round
    n_kv = n_steps - n_q
    head_dim = width // 2
    half_dim = head_dim // 2
    blk_q = s_buf.shape[1] // 2
    blk_k = s_buf.shape[0]
    n_blocks = total // blk_q
    ratio = blk_k // blk_q
    span = blk_q // seq
    chips_per_k = blk_k // (2 * seq)
    factor = LOG2E * head_dim ** -0.5

    def kv_block(step):
        return lax.rem(step + chip, n_kv)

    def q_block(step):
        return lax.rem(step - n_kv + chip, n_q)

    def fetch(step, slot):
        @pl.when(step < n_kv)
        def _():
            cols = pl.ds(pl.multiple_of(kv_block(step) * head_dim, head_dim), head_dim)
            pltpu.make_async_copy(wk_ref.at[:, cols], w_buf.at[slot, :, pl.ds(0, head_dim)], w_sem.at[slot]).start()
            pltpu.make_async_copy(wv_ref.at[:, cols], w_buf.at[slot, :, pl.ds(head_dim, head_dim)], w_sem.at[slot]).start()

        @pl.when(step >= n_kv)
        def _():
            cols = pl.ds(pl.multiple_of(q_block(step) * width, width), width)
            pltpu.make_async_copy(wq_ref.at[:, cols], w_buf.at[slot], w_sem.at[slot]).start()

    def send_kv_tiles(step, first, last):
        for b in range(first * per_round, last * per_round):
            owner = 2 * (b % per_round * n_kv + kv_block(step)) + core
            r = b // per_round
            put(stage.at[step, b], kv_in.at[r, chip, core], owner, me, send_kv, recv_kv.at[r])

    def send_q_tiles(step, r):
        for k in range(per_round):
            put(stage.at[step, r * per_round + k], q_in.at[r, pl.ds(me * seq, seq)], k * n_q + q_block(step), me, send_q, recv_q.at[r])

    early = min(2, rounds)

    def send_first(step):
        @pl.when(step < n_kv)
        def _():
            send_kv_tiles(step, 0, early)

        @pl.when(step >= n_kv)
        def _():
            send_q_tiles(step, 0)

        @pl.when((step >= n_kv) & (lax.rem(step, 2) == 1) & ((step - n_kv) // 2 < n_kv))
        def _():
            send_kv_tiles((step - n_kv) // 2, early, rounds)

    fetch(0, 0)
    group_signal(me, n_cp)

    def norm(k, _):
        rows = pl.ds(pl.multiple_of(k * NORM_ROWS, NORM_ROWS), NORM_ROWS)
        x = x_ref[rows, :].astype(jnp.float32)
        inv_rms = lax.rsqrt(jnp.mean(x * x, axis=-1, keepdims=True) + 1e-5)
        h_ref[rows, :] = (x * inv_rms * gain_ref[...].astype(jnp.float32).reshape(1, gain_ref.shape[0])).astype(jnp.bfloat16)
        return 0

    lax.fori_loop(0, batch * seq // NORM_ROWS, norm, 0)
    pl.semaphore_wait(pltpu.get_barrier_semaphore(), n_cp - 1)

    def rotate(x):
        return (x * cos_ref[...] + pltpu.roll(x, half_dim, 1) * sin_ref[...]).astype(jnp.bfloat16).reshape(batch, seq, head_dim)

    def project(step, _):
        slot = lax.rem(step, 2)
        wait_bytes_of(w_buf.at[slot], w_sem.at[slot])

        @pl.when(step + 1 < n_steps)
        def _():
            fetch(step + 1, 1 - slot)

        acc[...] = jnp.dot(h_ref[...], w_buf[slot], preferred_element_type=jnp.float32)
        stage[step, :, :, 0:head_dim] = rotate(acc[:, 0:head_dim])

        @pl.when(step < n_kv)
        def _():
            stage[step, :, :, head_dim:width] = acc[:, head_dim:width].astype(jnp.bfloat16).reshape(batch, seq, head_dim)

        @pl.when(step >= n_kv)
        def _():
            stage[step, :, :, head_dim:width] = rotate(acc[:, head_dim:width])

        @pl.when(step > 0)
        def _():
            send_first(step - 1)

        return 0

    lax.fori_loop(0, n_steps, project, 0)
    send_first(n_steps - 1)

    def swap(r, _):
        wait_bytes_of(kv_in.at[r, :, 0], recv_kv.at[r])
        mine = kv_in.at[r, :, core]
        pltpu.make_async_remote_copy(mine, mine, send_half, recv_half.at[r], device_id={AXIS: me + 1 - 2 * core}, device_id_type=pl.DeviceIdType.MESH).start()
        return 0

    lax.fori_loop(0, early, swap, 0)

    def send_rest(k, _):
        send_q_tiles(n_kv + lax.rem(k, n_q), 1 + k // n_q)
        return 0

    lax.fori_loop(0, (rounds - 1) * n_q, send_rest, 0)

    def out_fetch(k, slot):
        cols = pl.ds(pl.multiple_of(lax.rem(k, n_out) * width, width), width)
        pltpu.make_async_copy(wo_ref.at[:, cols], w_buf.at[slot], w_sem.at[slot]).start()

    n_out = wo_ref.shape[1] // width
    out_fetch(0, 0)

    def place(t):
        i = lax.rem(t + me // span + 1, n_blocks)
        return i, i // ratio

    def attend(r, _):
        @pl.when((r + 1 >= early) & (r + 1 < rounds))
        def _():
            swap(r + 1, 0)

        wait_bytes_of(q_in.at[r], recv_q.at[r])
        wait_bytes_of(kv_in.at[r, :, 0], recv_half.at[r])

        def kv_rows(j, lanes):
            return kv_in[r, pl.ds(j * chips_per_k, chips_per_k), :, :, lanes].reshape(blk_k, head_dim)

        def turn(j, _):
            v_t[:, pl.ds(pl.multiple_of(j * blk_k, blk_k), blk_k)] = kv_rows(j, slice(head_dim, width)).astype(jnp.float32).T.astype(jnp.bfloat16)
            return 0

        lax.fori_loop(0, total // blk_k, turn, 0)

        def send(t):
            i, _ = place(t)
            b = r * per_round + me // n_q
            cols = pl.ds(pl.multiple_of(lax.rem(me, n_q) * width, width), width)
            for s in range(span):
                owner = i * span + s
                put(o_stage.at[r, pl.ds(owner * seq, seq)], o_in.at[b, :, cols], owner, me, send_o, recv_o.at[r])

        def next_scores(i, j):
            k_blk = kv_rows(j, slice(0, head_dim))
            q_rows = pl.ds(pl.multiple_of(i * blk_q, blk_q), blk_q)
            for g in range(2):
                q_head = q_in[r, q_rows, g * head_dim:(g + 1) * head_dim]
                cols = slice(g * blk_q, (g + 1) * blk_q)
                s = lax.dot_general(k_blk, q_head, (((1,), (1,)), ((), ())), preferred_element_type=jnp.float32)
                s_buf[:, cols] = s
                stat[3, 0:1, cols] = jnp.max(s, axis=0, keepdims=True)

        def weighed(j):
            cols = pl.ds(pl.multiple_of(j * blk_k, blk_k), blk_k)
            return o_acc[...] * stat[2, 0:1, :] + jnp.dot(v_t[:, cols], p_buf[...], preferred_element_type=jnp.float32)

        def finish(t):
            i, n_full = place(t)
            out = weighed(jnp.maximum(n_full - 1, 0)) * (1.0 / stat[1, 0:1, :])
            q_rows = pl.ds(pl.multiple_of(i * blk_q, blk_q), blk_q)
            for g in range(2):
                o_stage[r, q_rows, g * head_dim:(g + 1) * head_dim] = out[:, g * blk_q:(g + 1) * blk_q].T.astype(jnp.bfloat16)

        def step(t, _):
            i, n_full = place(t)
            after = place(jnp.minimum(t + 1, n_blocks - 1))

            def follow(n_done):
                more = n_done < n_full
                next_scores(jnp.where(more, i, after[0]), jnp.where(more, n_done, after[1]))

            @pl.when(t > 1)
            def _():
                send(t - 2)

            def diagonal(size):
                finish(jnp.maximum(t - 1, 0))
                o_acc[...] = jnp.zeros_like(o_acc)
                shape = (size, 2 * blk_q)
                allowed = lax.broadcasted_iota(jnp.int32, shape, 0) - (size - blk_q) <= lax.rem(lax.broadcasted_iota(jnp.int32, shape, 1), blk_q)
                s = jnp.where(allowed, s_buf[0:size, :], -jnp.inf)
                top = jnp.max(s, axis=0, keepdims=True)
                prob = jnp.exp2(s * factor - top * factor)
                stat[0, 0:1, :] = top
                stat[1, 0:1, :] = jnp.sum(prob, axis=0, keepdims=True)
                stat[2, 0:1, :] = jnp.ones_like(top)
                p_buf[0:size, :] = prob.astype(jnp.bfloat16)
                if size < blk_k:
                    p_buf[size:blk_k, :] = jnp.zeros((blk_k - size, 2 * blk_q), jnp.bfloat16)
                follow(0)

            for part in range(ratio):
                pl.when(lax.rem(i, ratio) == part)(functools.partial(diagonal, (part + 1) * blk_q))

            def full(j, _):
                o_acc[...] = weighed(jnp.where(j == 0, n_full, j - 1))
                top = stat[0, 0:1, :]
                new_top = jnp.maximum(top, stat[3, 0:1, :])
                shift = new_top * factor
                rescale = jnp.exp2(top * factor - shift)
                part_sum = jnp.zeros((8, 2 * blk_q), jnp.float32)
                for k in range(0, blk_k, CHUNK):
                    prob = jnp.exp2(s_buf[k:k + CHUNK, :] * factor - shift)
                    part_sum = part_sum + jnp.sum(prob.reshape(CHUNK // 8, 8, 2 * blk_q), axis=0)
                    p_buf[k:k + CHUNK, :] = prob.astype(jnp.bfloat16)
                stat[0, 0:1, :] = new_top
                stat[1, 0:1, :] = stat[1, 0:1, :] * rescale + jnp.sum(part_sum, axis=0, keepdims=True)
                stat[2, 0:1, :] = rescale
                follow(j + 1)
                return 0

            lax.fori_loop(0, n_full, full, 0)
            return 0

        o_acc[...] = jnp.zeros_like(o_acc)
        stat[...] = jnp.ones_like(stat)
        p_buf[...] = jnp.zeros_like(p_buf)
        next_scores(*place(0))
        lax.fori_loop(0, n_blocks, step, 0)
        send(n_blocks - 2)
        finish(n_blocks - 1)
        send(n_blocks - 1)
        return 0

    lax.fori_loop(0, rounds, attend, 0)

    def y_copy(k, slot):
        r, cols = k // n_out, pl.ds(pl.multiple_of(lax.rem(k, n_out) * width, width), width)
        return pltpu.make_async_copy(y_buf.at[slot], y_ref.at[pl.ds(r * per_round, per_round), :, cols], y_sem.at[slot])

    def out_project(k, _):
        slot, r = lax.rem(k, 2), k // n_out

        @pl.when(k + 1 < rounds * n_out)
        def _():
            out_fetch(k + 1, 1 - slot)

        @pl.when(lax.rem(k, n_out) == 0)
        def _():
            wait_bytes_of(o_in.at[pl.ds(r * per_round, per_round)], recv_o.at[r])

        wait_bytes_of(w_buf.at[slot], w_sem.at[slot])

        @pl.when(k > 1)
        def _():
            y_copy(k - 2, slot).wait()

        attn = o_in[pl.ds(r * per_round, per_round)].reshape(per_round * seq, wo_ref.shape[0])
        proj = jnp.dot(attn, w_buf[slot], preferred_element_type=jnp.float32)
        rows = pl.ds(pl.multiple_of(r * per_round * seq, seq), per_round * seq)
        cols = pl.ds(pl.multiple_of(lax.rem(k, n_out) * width, width), width)
        y_buf[slot] = (x_ref[rows, cols].astype(jnp.float32) + proj).astype(jnp.bfloat16).reshape(per_round, seq, width)
        y_copy(k, slot).start()
        return 0

    lax.fori_loop(0, rounds * n_out, out_project, 0)
    for k in (rounds * n_out - 2, rounds * n_out - 1):
        y_copy(k, k % 2).wait()
    away = (n_cp - 1) * seq
    wait_bytes_of(q_in.at[:, pl.ds(0, away)], send_q)
    wait_bytes_of(kv_in.at[:, pl.ds(0, n_cp // 2 - 1), 0], send_kv)
    wait_bytes_of(o_stage.at[:, pl.ds(0, away)], send_o)
    wait_bytes_of(kv_in.at[:, :, 0], send_half)


def solution(mesh):
    n_cp = mesh.shape[AXIS]

    def local_block(hidden, positions, norm_gain, w_query, w_key, w_value, w_out):
        batch, seq, model_dim = hidden.shape
        n_heads, head_dim, _ = w_out.shape
        n_kv = w_key.shape[1] // head_dim
        width = 2 * head_dim
        n_q = n_heads // 2
        rounds = batch * n_q // n_cp
        per_round = batch // rounds
        total = n_cp * seq
        n_steps = n_kv + n_q
        blk_q = 4 * seq
        blk_k = blk_q
        any_space = pl.BlockSpec(memory_space=pl.ANY)
        vmem = pl.BlockSpec(memory_space=pltpu.VMEM)
        cos_tab, sin_tab = rotary_tables(positions, head_dim)
        dma = pltpu.SemaphoreType.DMA
        return pl.pallas_call(
            functools.partial(block_kernel, n_cp),
            out_shape=jax.ShapeDtypeStruct(hidden.shape, jnp.bfloat16),
            in_specs=[vmem] * 4 + [any_space] * 4,
            out_specs=any_space,
            scratch_shapes=[
                pltpu.VMEM((batch * seq, model_dim), jnp.bfloat16),
                pltpu.VMEM((2, model_dim, width), jnp.bfloat16),
                pltpu.VMEM((batch * seq, width), jnp.float32),
                pltpu.VMEM((n_steps, batch, seq, width), jnp.bfloat16),
                pltpu.VMEM((rounds, total, width), jnp.bfloat16),
                pltpu.VMEM((rounds, n_cp // 2, 2, seq, width), jnp.bfloat16),
                pltpu.VMEM((head_dim, total), jnp.bfloat16),
                pltpu.VMEM((rounds, total, width), jnp.bfloat16),
                pltpu.VMEM((blk_k, 2 * blk_q), jnp.float32),
                pltpu.VMEM((blk_k, 2 * blk_q), jnp.bfloat16),
                pltpu.VMEM((head_dim, 2 * blk_q), jnp.float32),
                pltpu.VMEM((4, 8, 2 * blk_q), jnp.float32),
                pltpu.VMEM((batch, seq, n_heads * head_dim), jnp.bfloat16),
                pltpu.VMEM((2, per_round, seq, width), jnp.bfloat16),
                dma((2,)), dma((2,)),
                dma, dma, dma, dma,
                dma((rounds,)), dma((rounds,)), dma((rounds,)), dma((rounds,)),
            ],
            compiler_params=pltpu.CompilerParams(collective_id=0, has_side_effects=True, vmem_limit_bytes=VMEM_LIMIT),
            name='attention_block',
        )(hidden.reshape(batch * seq, model_dim), norm_gain, cos_tab, sin_tab, w_query, w_key, w_value, w_out.reshape(n_heads * head_dim, model_dim))

    act_spec = P('dp', 'cp', None)
    return jax.shard_map(local_block, mesh=mesh, in_specs=(act_spec, P('dp', 'cp'), P(), P(), P(), P(), P()), out_specs=act_spec, check_vma=False)
```

```python
import functools

import jax
import jax.numpy as jnp
from jax import lax
from jax.experimental import pallas as pl
from jax.experimental.pallas import tpu as pltpu
from jax.sharding import PartitionSpec as P

AXIS = 'cp'
LOG2E = 1.4426950408889634
CHUNK = 32
NORM_ROWS = 32
VMEM_LIMIT = 60 * 1024 * 1024


def cos_sin(angles):
    quarter = jnp.round(angles * 0.6366197723675814)
    rest = ((angles - quarter * 1.5703125) - quarter * 4.837512969970703e-4) - quarter * 7.549789954891626e-8
    square = rest * rest
    sin_poly = rest + rest * square * (-1.6666654611e-1 + square * (8.3321608736e-3 - square * 1.9515295891e-4))
    cos_poly = 1.0 - 0.5 * square + square * square * (4.166664568298827e-2 + square * (-1.388731625493765e-3 + square * 2.443315711809948e-5))
    turn = quarter.astype(jnp.int32) & 3
    odd = (turn & 1) == 1
    cos_part = jnp.where(odd, sin_poly, cos_poly)
    sin_part = jnp.where(odd, cos_poly, sin_poly)
    return jnp.where((turn == 1) | (turn == 2), -cos_part, cos_part), jnp.where(turn >= 2, -sin_part, sin_part)


def rotary_tables(positions, head_dim):
    half_dim = head_dim // 2
    inv_freq = 10000.0 ** (-2.0 * jnp.arange(half_dim, dtype=jnp.float32) / head_dim)
    sign = jnp.where(jnp.arange(head_dim) < half_dim, -1.0, 1.0).astype(jnp.float32)
    angles = positions.reshape(-1, 1).astype(jnp.float32) * jnp.concatenate([inv_freq, inv_freq])
    cos_tab, sin_tab = cos_sin(angles)
    return cos_tab, sin_tab * sign


def group_signal(me, n_cp):
    barrier = pltpu.get_barrier_semaphore()

    def signal(k, _):
        pl.semaphore_signal(barrier, inc=1, device_id={AXIS: lax.rem(me + k, n_cp)}, device_id_type=pl.DeviceIdType.MESH)
        return 0

    lax.fori_loop(1, n_cp, signal, 0)


def put(src, dst, owner, me, send_sem, recv_sem):
    @pl.when(owner == me)
    def _():
        pltpu.make_async_copy(src, dst, recv_sem).start()

    @pl.when(owner != me)
    def _():
        pltpu.make_async_remote_copy(src, dst, send_sem, recv_sem, device_id={AXIS: owner}, device_id_type=pl.DeviceIdType.MESH).start()


def wait_bytes_of(ref, sem):
    pltpu.make_async_copy(ref, ref, sem).wait()


def block_kernel(
    n_cp, x_ref, gain_ref, cos_ref, sin_ref, wq_ref, wk_ref, wv_ref, wo_ref, y_ref,
    h_ref, w_buf, acc, stage, q_in, kv_in, v_t, o_stage, s_buf, p_buf, o_acc, stat, o_in, y_buf,
    w_sem, y_sem, send_q, send_kv, send_o, send_half, recv_q, recv_kv, recv_o, recv_half,
):
    me = lax.axis_index(AXIS)
    chip, core = me // 2, lax.rem(me, 2)
    n_steps, batch, seq, width = stage.shape
    rounds, total, _ = q_in.shape
    per_round = batch // rounds
    n_q = n_cp // per_round
    n_kv = n_steps - n_q
    head_dim = width // 2
    half_dim = head_dim // 2
    blk_q = s_buf.shape[1] // 2
    blk_k = s_buf.shape[0]
    n_blocks = total // blk_q
    ratio = blk_k // blk_q
    span = blk_q // seq
    chips_per_k = blk_k // (2 * seq)
    factor = LOG2E * head_dim ** -0.5

    def kv_block(step):
        return lax.rem(step + chip, n_kv)

    def q_block(step):
        return lax.rem(step - n_kv + chip, n_q)

    def fetch(step, slot):
        @pl.when(step < n_kv)
        def _():
            cols = pl.ds(pl.multiple_of(kv_block(step) * head_dim, head_dim), head_dim)
            pltpu.make_async_copy(wk_ref.at[:, cols], w_buf.at[slot, :, pl.ds(0, head_dim)], w_sem.at[slot]).start()
            pltpu.make_async_copy(wv_ref.at[:, cols], w_buf.at[slot, :, pl.ds(head_dim, head_dim)], w_sem.at[slot]).start()

        @pl.when(step >= n_kv)
        def _():
            cols = pl.ds(pl.multiple_of(q_block(step) * width, width), width)
            pltpu.make_async_copy(wq_ref.at[:, cols], w_buf.at[slot], w_sem.at[slot]).start()

    def send_kv_tiles(step, first, last):
        for b in range(first * per_round, last * per_round):
            owner = 2 * (b % per_round * n_kv + kv_block(step)) + core
            r = b // per_round
            put(stage.at[step, b], kv_in.at[r, chip, core], owner, me, send_kv, recv_kv.at[r])

    def send_q_tiles(step, r):
        for k in range(per_round):
            put(stage.at[step, r * per_round + k], q_in.at[r, pl.ds(me * seq, seq)], k * n_q + q_block(step), me, send_q, recv_q.at[r])

    early = min(2, rounds)

    def send_first(step):
        @pl.when(step < n_kv)
        def _():
            send_kv_tiles(step, 0, early)

        @pl.when(step >= n_kv)
        def _():
            send_q_tiles(step, 0)

    fetch(0, 0)
    group_signal(me, n_cp)

    def norm(k, _):
        rows = pl.ds(pl.multiple_of(k * NORM_ROWS, NORM_ROWS), NORM_ROWS)
        x = x_ref[rows, :].astype(jnp.float32)
        inv_rms = lax.rsqrt(jnp.mean(x * x, axis=-1, keepdims=True) + 1e-5)
        h_ref[rows, :] = (x * inv_rms * gain_ref[...].astype(jnp.float32).reshape(1, gain_ref.shape[0])).astype(jnp.bfloat16)
        return 0

    lax.fori_loop(0, batch * seq // NORM_ROWS, norm, 0)
    pl.semaphore_wait(pltpu.get_barrier_semaphore(), n_cp - 1)

    def rotate(x):
        return (x * cos_ref[...] + pltpu.roll(x, half_dim, 1) * sin_ref[...]).astype(jnp.bfloat16).reshape(batch, seq, head_dim)

    def project(step, _):
        slot = lax.rem(step, 2)
        wait_bytes_of(w_buf.at[slot], w_sem.at[slot])

        @pl.when(step + 1 < n_steps)
        def _():
            fetch(step + 1, 1 - slot)

        acc[...] = jnp.dot(h_ref[...], w_buf[slot], preferred_element_type=jnp.float32)
        stage[step, :, :, 0:head_dim] = rotate(acc[:, 0:head_dim])

        @pl.when(step < n_kv)
        def _():
            stage[step, :, :, head_dim:width] = acc[:, head_dim:width].astype(jnp.bfloat16).reshape(batch, seq, head_dim)

        @pl.when(step >= n_kv)
        def _():
            stage[step, :, :, head_dim:width] = rotate(acc[:, head_dim:width])

        @pl.when(step > 0)
        def _():
            send_first(step - 1)

        return 0

    lax.fori_loop(0, n_steps, project, 0)
    send_first(n_steps - 1)

    def swap(r, _):
        wait_bytes_of(kv_in.at[r, :, 0], recv_kv.at[r])
        mine = kv_in.at[r, :, core]
        pltpu.make_async_remote_copy(mine, mine, send_half, recv_half.at[r], device_id={AXIS: me + 1 - 2 * core}, device_id_type=pl.DeviceIdType.MESH).start()
        return 0

    lax.fori_loop(0, early, swap, 0)

    def send_rest(k, _):
        send_q_tiles(n_kv + lax.rem(k, n_q), 1 + k // n_q)

        @pl.when(k < n_kv)
        def _():
            send_kv_tiles(k, early, rounds)

        return 0

    lax.fori_loop(0, (rounds - 1) * n_q, send_rest, 0)

    def out_fetch(k, slot):
        cols = pl.ds(pl.multiple_of(lax.rem(k, n_out) * width, width), width)
        pltpu.make_async_copy(wo_ref.at[:, cols], w_buf.at[slot], w_sem.at[slot]).start()

    n_out = wo_ref.shape[1] // width
    out_fetch(0, 0)

    def place(t):
        i = lax.rem(t + me // span + 1, n_blocks)
        return i, i // ratio

    def attend(r, _):
        @pl.when((r + 1 >= early) & (r + 1 < rounds))
        def _():
            swap(r + 1, 0)

        wait_bytes_of(q_in.at[r], recv_q.at[r])
        wait_bytes_of(kv_in.at[r, :, 0], recv_half.at[r])

        def kv_rows(j, lanes):
            return kv_in[r, pl.ds(j * chips_per_k, chips_per_k), :, :, lanes].reshape(blk_k, head_dim)

        def turn(j, _):
            v_t[:, pl.ds(pl.multiple_of(j * blk_k, blk_k), blk_k)] = kv_rows(j, slice(head_dim, width)).astype(jnp.float32).T.astype(jnp.bfloat16)
            return 0

        lax.fori_loop(0, total // blk_k, turn, 0)

        def send(t):
            i, _ = place(t)
            b = r * per_round + me // n_q
            cols = pl.ds(pl.multiple_of(lax.rem(me, n_q) * width, width), width)
            for s in range(span):
                owner = i * span + s
                put(o_stage.at[r, pl.ds(owner * seq, seq)], o_in.at[b, :, cols], owner, me, send_o, recv_o.at[r])

        def next_scores(i, j):
            k_blk = kv_rows(j, slice(0, head_dim))
            q_rows = pl.ds(pl.multiple_of(i * blk_q, blk_q), blk_q)
            for g in range(2):
                q_head = q_in[r, q_rows, g * head_dim:(g + 1) * head_dim]
                cols = slice(g * blk_q, (g + 1) * blk_q)
                s = lax.dot_general(k_blk, q_head, (((1,), (1,)), ((), ())), preferred_element_type=jnp.float32)
                s_buf[:, cols] = s
                stat[3, 0:1, cols] = jnp.max(s, axis=0, keepdims=True)

        def weighed(j):
            cols = pl.ds(pl.multiple_of(j * blk_k, blk_k), blk_k)
            return o_acc[...] * stat[2, 0:1, :] + jnp.dot(v_t[:, cols], p_buf[...], preferred_element_type=jnp.float32)

        def finish(t):
            i, n_full = place(t)
            out = weighed(jnp.maximum(n_full - 1, 0)) * (1.0 / stat[1, 0:1, :])
            q_rows = pl.ds(pl.multiple_of(i * blk_q, blk_q), blk_q)
            for g in range(2):
                o_stage[r, q_rows, g * head_dim:(g + 1) * head_dim] = out[:, g * blk_q:(g + 1) * blk_q].T.astype(jnp.bfloat16)

        def step(t, _):
            i, n_full = place(t)
            after = place(jnp.minimum(t + 1, n_blocks - 1))

            def follow(n_done):
                more = n_done < n_full
                next_scores(jnp.where(more, i, after[0]), jnp.where(more, n_done, after[1]))

            @pl.when(t > 1)
            def _():
                send(t - 2)

            def diagonal(size):
                finish(jnp.maximum(t - 1, 0))
                o_acc[...] = jnp.zeros_like(o_acc)
                shape = (size, 2 * blk_q)
                allowed = lax.broadcasted_iota(jnp.int32, shape, 0) - (size - blk_q) <= lax.rem(lax.broadcasted_iota(jnp.int32, shape, 1), blk_q)
                s = jnp.where(allowed, s_buf[0:size, :], -jnp.inf)
                top = jnp.max(s, axis=0, keepdims=True)
                prob = jnp.exp2(s * factor - top * factor)
                stat[0, 0:1, :] = top
                stat[1, 0:1, :] = jnp.sum(prob, axis=0, keepdims=True)
                stat[2, 0:1, :] = jnp.ones_like(top)
                p_buf[0:size, :] = prob.astype(jnp.bfloat16)
                if size < blk_k:
                    p_buf[size:blk_k, :] = jnp.zeros((blk_k - size, 2 * blk_q), jnp.bfloat16)
                follow(0)

            for part in range(ratio):
                pl.when(lax.rem(i, ratio) == part)(functools.partial(diagonal, (part + 1) * blk_q))

            def full(j, _):
                o_acc[...] = weighed(jnp.where(j == 0, n_full, j - 1))
                top = stat[0, 0:1, :]
                new_top = jnp.maximum(top, stat[3, 0:1, :])
                shift = new_top * factor
                rescale = jnp.exp2(top * factor - shift)
                part_sum = jnp.zeros((8, 2 * blk_q), jnp.float32)
                for k in range(0, blk_k, CHUNK):
                    prob = jnp.exp2(s_buf[k:k + CHUNK, :] * factor - shift)
                    part_sum = part_sum + jnp.sum(prob.reshape(CHUNK // 8, 8, 2 * blk_q), axis=0)
                    p_buf[k:k + CHUNK, :] = prob.astype(jnp.bfloat16)
                stat[0, 0:1, :] = new_top
                stat[1, 0:1, :] = stat[1, 0:1, :] * rescale + jnp.sum(part_sum, axis=0, keepdims=True)
                stat[2, 0:1, :] = rescale
                follow(j + 1)
                return 0

            lax.fori_loop(0, n_full, full, 0)
            return 0

        o_acc[...] = jnp.zeros_like(o_acc)
        stat[...] = jnp.ones_like(stat)
        p_buf[...] = jnp.zeros_like(p_buf)
        next_scores(*place(0))
        lax.fori_loop(0, n_blocks, step, 0)
        send(n_blocks - 2)
        finish(n_blocks - 1)
        send(n_blocks - 1)
        return 0

    lax.fori_loop(0, rounds, attend, 0)

    def y_copy(k, slot):
        r, cols = k // n_out, pl.ds(pl.multiple_of(lax.rem(k, n_out) * width, width), width)
        return pltpu.make_async_copy(y_buf.at[slot], y_ref.at[pl.ds(r * per_round, per_round), :, cols], y_sem.at[slot])

    def out_project(k, _):
        slot, r = lax.rem(k, 2), k // n_out

        @pl.when(k + 1 < rounds * n_out)
        def _():
            out_fetch(k + 1, 1 - slot)

        @pl.when(lax.rem(k, n_out) == 0)
        def _():
            wait_bytes_of(o_in.at[pl.ds(r * per_round, per_round)], recv_o.at[r])

        wait_bytes_of(w_buf.at[slot], w_sem.at[slot])

        @pl.when(k > 1)
        def _():
            y_copy(k - 2, slot).wait()

        attn = o_in[pl.ds(r * per_round, per_round)].reshape(per_round * seq, wo_ref.shape[0])
        proj = jnp.dot(attn, w_buf[slot], preferred_element_type=jnp.float32)
        rows = pl.ds(pl.multiple_of(r * per_round * seq, seq), per_round * seq)
        cols = pl.ds(pl.multiple_of(lax.rem(k, n_out) * width, width), width)
        y_buf[slot] = (x_ref[rows, cols].astype(jnp.float32) + proj).astype(jnp.bfloat16).reshape(per_round, seq, width)
        y_copy(k, slot).start()
        return 0

    lax.fori_loop(0, rounds * n_out, out_project, 0)
    for k in (rounds * n_out - 2, rounds * n_out - 1):
        y_copy(k, k % 2).wait()
    away = (n_cp - 1) * seq
    wait_bytes_of(q_in.at[:, pl.ds(0, away)], send_q)
    wait_bytes_of(kv_in.at[:, pl.ds(0, n_cp // 2 - 1), 0], send_kv)
    wait_bytes_of(o_stage.at[:, pl.ds(0, away)], send_o)
    wait_bytes_of(kv_in.at[:, :, 0], send_half)


def solution(mesh):
    n_cp = mesh.shape[AXIS]

    def local_block(hidden, positions, norm_gain, w_query, w_key, w_value, w_out):
        batch, seq, model_dim = hidden.shape
        n_heads, head_dim, _ = w_out.shape
        n_kv = w_key.shape[1] // head_dim
        width = 2 * head_dim
        n_q = n_heads // 2
        rounds = batch * n_q // n_cp
        per_round = batch // rounds
        total = n_cp * seq
        n_steps = n_kv + n_q
        blk_q = 4 * seq
        blk_k = blk_q
        any_space = pl.BlockSpec(memory_space=pl.ANY)
        vmem = pl.BlockSpec(memory_space=pltpu.VMEM)
        cos_tab, sin_tab = rotary_tables(positions, head_dim)
        dma = pltpu.SemaphoreType.DMA
        return pl.pallas_call(
            functools.partial(block_kernel, n_cp),
            out_shape=jax.ShapeDtypeStruct(hidden.shape, jnp.bfloat16),
            in_specs=[vmem] * 4 + [any_space] * 4,
            out_specs=any_space,
            scratch_shapes=[
                pltpu.VMEM((batch * seq, model_dim), jnp.bfloat16),
                pltpu.VMEM((2, model_dim, width), jnp.bfloat16),
                pltpu.VMEM((batch * seq, width), jnp.float32),
                pltpu.VMEM((n_steps, batch, seq, width), jnp.bfloat16),
                pltpu.VMEM((rounds, total, width), jnp.bfloat16),
                pltpu.VMEM((rounds, n_cp // 2, 2, seq, width), jnp.bfloat16),
                pltpu.VMEM((head_dim, total), jnp.bfloat16),
                pltpu.VMEM((rounds, total, width), jnp.bfloat16),
                pltpu.VMEM((blk_k, 2 * blk_q), jnp.float32),
                pltpu.VMEM((blk_k, 2 * blk_q), jnp.bfloat16),
                pltpu.VMEM((head_dim, 2 * blk_q), jnp.float32),
                pltpu.VMEM((4, 8, 2 * blk_q), jnp.float32),
                pltpu.VMEM((batch, seq, n_heads * head_dim), jnp.bfloat16),
                pltpu.VMEM((2, per_round, seq, width), jnp.bfloat16),
                dma((2,)), dma((2,)),
                dma, dma, dma, dma,
                dma((rounds,)), dma((rounds,)), dma((rounds,)), dma((rounds,)),
            ],
            compiler_params=pltpu.CompilerParams(collective_id=0, has_side_effects=True, vmem_limit_bytes=VMEM_LIMIT),
            name='attention_block',
        )(hidden.reshape(batch * seq, model_dim), norm_gain, cos_tab, sin_tab, w_query, w_key, w_value, w_out.reshape(n_heads * head_dim, model_dim))

    act_spec = P('dp', 'cp', None)
    return jax.shard_map(local_block, mesh=mesh, in_specs=(act_spec, P('dp', 'cp'), P(), P(), P(), P(), P()), out_specs=act_spec, check_vma=False)
```
